128 devices in a mesh: seq: 32 (over x, z, core), head: 4 (over y).
Axes of the slice: x: 4, y: 4, z: 4, core: 2. Of those that a mesh axis runs over, the one named last changes fastest.
Arguments:
- tokens: bfloat16 [2, 16384, 2560], P(None, 'seq'), may hold values from -6 to 6
- gate_weight: bfloat16 [2560, 5120], P(None, 'head'), may hold values from -0.125 to 0.125
- value_weight: bfloat16 [2560, 5120], P(None, 'head'), may hold values from -0.125 to 0.125
- state_weight: bfloat16 [2560, 256], replicated, may hold values from -0.125 to 0.125
- step_weight: bfloat16 [2560, 80], P(None, 'head'), may hold values from -0.125 to 0.125
- value_kernel: float32 [4, 5120], P(None, 'head'), may hold values from -3 to 3
- value_offset: float32 [5120], P('head'), may hold values from -3 to 3
- state_kernel: float32 [4, 256], replicated, may hold values from -3 to 3
- state_offset: float32 [256], replicated, may hold values from -3 to 3
- step_offset: float32 [80], P('head'), may hold values from -2 to 0.5
- decay_rate: float32 [80], P('head'), may hold values from 6.1035156e-05 to 0.1
- skip_gain: float32 [80], P('head'), may hold values from 0.5 to 2
- norm_gain: float32 [5120], P('head'), may hold values from 0.5 to 1.5
Outputs:
- normed: bfloat16 [2, 16384, 5120], P(None, 'seq', 'head')
The draws below stay inside these ranges and needn't reach their ends.
All inputs are finite; a program needn't handle non-finite values.
Results may differ from the reference program's by a relative error of at most 0.0054.
Values may be sent and summed in bfloat16 or wider, within the bound.
A program may use at most 128 MiB of HBM per device.

```python
import math
import jax
import jax.numpy as jnp
from jax import lax

D = 2560
HEADS = 80
HEAD_DIM = 64
STATE = 128
WIDTH = 4
GROUP = 256
BATCH = 2
SEQLEN = 16384
INNER = 5120


def steps_of(stream_key, shape, shards, least, top_value):
    loudness, own = 1.0, jax.random.fold_in(stream_key, 6)
    for position, parts in shards:
        heights = jnp.exp(jax.random.uniform(jax.random.fold_in(own, position), (parts,), jnp.float32, least / len(shards), top_value / len(shards)))
        loudness = loudness * jnp.repeat(heights, shape[position] // parts).reshape([-1 if axis == position else 1 for axis in range(len(shape))])
    return loudness


def scatter_about(stream_key, shape, scale, reach, pieces=(), kind=jnp.bfloat16):
    drawn = scale * jax.random.normal(stream_key, shape, jnp.float32)
    if pieces:
        drawn = drawn * steps_of(stream_key, shape, pieces, -0.22, 0.18)
    return jnp.clip(drawn, -reach, reach).astype(kind)


def setup_inputs(seed: int = 0) -> dict:
    arg_keys = jax.random.split(jax.random.key(seed), 14)
    tokens = scatter_about(arg_keys[0], (BATCH, SEQLEN, D), 1.0, 6.0, ((1, 32),))
    gate_weight = scatter_about(arg_keys[1], (D, INNER), D ** -0.5, 0.125, ((1, 4),))
    value_weight = scatter_about(arg_keys[2], (D, INNER), D ** -0.5, 0.125, ((1, 4),))
    state_weight = scatter_about(arg_keys[3], (D, 2 * STATE), D ** -0.5, 0.125)
    step_weight = scatter_about(arg_keys[4], (D, HEADS), D ** -0.5, 0.125, ((1, 4),))
    value_kernel = scatter_about(arg_keys[5], (WIDTH, INNER), WIDTH ** -0.5, 3.0, ((1, 4),), jnp.float32)
    value_offset = scatter_about(arg_keys[6], (INNER,), 0.5, 3.0, ((0, 4),), jnp.float32)
    state_kernel = scatter_about(arg_keys[7], (WIDTH, 2 * STATE), WIDTH ** -0.5, 3.0, (), jnp.float32)
    state_offset = scatter_about(arg_keys[8], (2 * STATE,), 0.5, 3.0, (), jnp.float32)
    step_offset = jnp.clip(-2.0 + 2.5 * jax.random.uniform(arg_keys[9], (HEADS,), jnp.float32) ** steps_of(arg_keys[9], (HEADS,), ((0, 4),), -0.2, 0.2), -2.0, 0.5)
    decay_rate = jnp.clip(jnp.exp(math.log(0.1) - 7.4014754 * jax.random.uniform(arg_keys[10], (HEADS,), jnp.float32) ** steps_of(arg_keys[10], (HEADS,), ((0, 4),), -0.2, 0.2)), 6.103515625e-05, 0.1)
    skip_gain = jnp.clip(0.5 + 1.5 * jax.random.uniform(arg_keys[11], (HEADS,), jnp.float32) ** steps_of(arg_keys[11], (HEADS,), ((0, 4),), -0.2, 0.2), 0.5, 2.0)
    norm_gain = jnp.clip(1.0 + 0.1 * jax.random.normal(arg_keys[12], (INNER,), jnp.float32), 0.5, 1.5)
    return dict(tokens=tokens, gate_weight=gate_weight, value_weight=value_weight, state_weight=state_weight, step_weight=step_weight, value_kernel=value_kernel, value_offset=value_offset, state_kernel=state_kernel, state_offset=state_offset, step_offset=step_offset, decay_rate=decay_rate, skip_gain=skip_gain, norm_gain=norm_gain)


EPS = 1e-05

def conv_rows(previous, incoming, kernel, offset):
    joined = jnp.concatenate([previous, incoming], axis=-2).astype(jnp.float32)
    length = incoming.shape[-2]
    axis_pos = joined.ndim - 2
    summed = offset + kernel[0] * lax.slice_in_dim(joined, 0, length, axis=axis_pos)
    for tap_index in range(1, kernel.shape[0]):
        summed = summed + kernel[tap_index] * lax.slice_in_dim(joined, tap_index, tap_index + length, axis=axis_pos)
    return jax.nn.silu(summed).astype(jnp.bfloat16)

def group_core(values, b_rows, c_rows, step_sizes, decay_rate):
    log_decay = -step_sizes * decay_rate
    cumulative = jnp.cumsum(log_decay, axis=0)
    length = step_sizes.shape[0]
    causal = (jnp.arange(length)[:, None] >= jnp.arange(length)[None, :])[:, :, None]
    scores = jnp.dot(c_rows, b_rows.T, preferred_element_type=jnp.float32)
    spread = jnp.where(causal, cumulative[:, None, :] - cumulative[None, :, :], 0.0)
    mixing = jnp.where(causal, scores[:, :, None] * jnp.exp(spread) * step_sizes[None, :, :], 0.0).astype(jnp.bfloat16)
    within = jnp.einsum('tsh,shp->thp', mixing.astype(jnp.float32), values.astype(jnp.float32))
    closing = jnp.exp(cumulative[-1][None, :] - cumulative) * step_sizes
    weighted = (closing[:, :, None] * b_rows.astype(jnp.float32)[:, None, :]).astype(jnp.bfloat16)
    produced = jnp.einsum('shp,shn->hpn', values.astype(jnp.float32), weighted.astype(jnp.float32))
    return (within, produced, jnp.exp(cumulative[-1]), jnp.exp(cumulative))

def reference(tokens, gate_weight, value_weight, state_weight, step_weight, value_kernel, value_offset, state_kernel, state_offset, step_offset, decay_rate, skip_gain, norm_gain):
    rim_rows = WIDTH - 1

    def advance(carried_in, token_block):
        memory, value_tail, inout_tail = carried_in
        gate_part = jnp.dot(token_block, gate_weight, preferred_element_type=jnp.float32).astype(jnp.bfloat16)
        values = jnp.dot(token_block, value_weight, preferred_element_type=jnp.float32).astype(jnp.bfloat16)
        inout_rows = jnp.dot(token_block, state_weight, preferred_element_type=jnp.float32).astype(jnp.bfloat16)
        step_sizes = jax.nn.softplus(jnp.dot(token_block, step_weight, preferred_element_type=jnp.float32) + step_offset)
        value_conv = conv_rows(value_tail, values, value_kernel, value_offset)
        inout_conv = conv_rows(inout_tail, inout_rows, state_kernel, state_offset)
        b_rows = inout_conv[:, :STATE]
        c_rows = inout_conv[:, STATE:]
        heads_view = value_conv.reshape(GROUP, HEADS, HEAD_DIM)
        within, produced, through, inside = group_core(heads_view, b_rows, c_rows, step_sizes, decay_rate)
        carried = jnp.einsum('tn,hpn->thp', c_rows.astype(jnp.float32), memory, precision=lax.Precision.HIGHEST)
        mixture = within + inside[:, :, None] * carried + skip_gain[None, :, None] * heads_view.astype(jnp.float32)
        gated_rows = mixture.reshape(GROUP, INNER) * jax.nn.silu(gate_part.astype(jnp.float32))
        inverse = lax.rsqrt(lax.optimization_barrier(jnp.mean(gated_rows * gated_rows, axis=-1, keepdims=True)) + EPS)
        output = (gated_rows * inverse * norm_gain).astype(jnp.bfloat16)
        memory = through[:, None, None] * memory + produced
        return ((memory, values[GROUP - rim_rows:], inout_rows[GROUP - rim_rows:]), output)

    def one_sequence(sequence_rows):
        blocks = sequence_rows.reshape(SEQLEN // GROUP, GROUP, D)
        initial = (jnp.zeros((HEADS, HEAD_DIM, STATE), jnp.float32), jnp.zeros((rim_rows, INNER), jnp.bfloat16), jnp.zeros((rim_rows, 2 * STATE), jnp.bfloat16))
        final_state, outputs = lax.scan(advance, initial, blocks)
        return outputs.reshape(SEQLEN, INNER)
    return lax.map(one_sequence, tokens)
```

```python
import functools

import jax
import jax.numpy as jnp
from jax import lax
from jax.experimental import pallas as pl
from jax.experimental.pallas import tpu as pltpu
from jax.sharding import PartitionSpec as P

MESH = pl.DeviceIdType.MESH
F32 = jnp.float32
BF16 = jnp.bfloat16

EPS = 1e-05
LOG2E = 1.4426950408889634
B = 2
T = 512
D = 2560
C = 1280
H = 20
N = 128
L = 128
K = T // L
GC = 256
G = C // GC
HALO = 16
R = T + HALO
TAPS = 4
PEERS = 32
HEADS_AXIS = 4
INNER = 5120


def dot(a, b):
    return jnp.dot(a, b, preferred_element_type=F32)


def split3(x):
    hi = x.astype(BF16).astype(F32)
    rest = x - hi
    mid = rest.astype(BF16).astype(F32)
    return hi, mid, rest - mid


def packed(x):
    lane = lax.broadcasted_iota(jnp.int32, x.shape, 1)
    hi, mid, low = split3(jnp.where(lane < H, x, 0.0))
    return (hi + pltpu.roll(mid, 32, 1) + pltpu.roll(low, 64, 1)).astype(BF16)


def silu(x):
    half = 0.5 * x
    return half * jnp.tanh(half) + half


def spread_matrix(shape, first_head, width):
    row = lax.broadcasted_iota(jnp.int32, shape, 0)
    col = lax.broadcasted_iota(jnp.int32, shape, 1)
    hit = (row & 31) == (first_head + col // width)
    return jnp.where(hit & (row < 96), 1.0, 0.0).astype(BF16)


def body(
    tok, gate_w, value_w, state_w, step_w,
    value_k, value_o, state_k, state_o, step_o, decay, skip, gain,
    out,
    x, wv, wg, ws, wd, cv, vbuf, gbuf, mixbuf, brow_t, crow, sc, a3, a2w, a2g, cs_t,
    e512, e256, eh, rows_t, rows_b, rows_s, pad, local, sendbuf, recvbuf, retbuf, retrecv,
    logsend, logrecv, fac, sq, ssend, srecv, obuf,
    xsem, vsem, gsem, msem, osem, hsem, ssem, rsem, tsem, usem, lsem, qsem,
):
    me = lax.axis_index("seq")
    hd = lax.axis_index("head")

    x_copies = [
        pltpu.make_async_copy(tok.at[b], x.at[b, pl.ds(HALO, T)], xsem.at[b]) for b in range(B)
    ]
    s_copy = pltpu.make_async_copy(state_w, ws, msem.at[0])
    d_copy = pltpu.make_async_copy(step_w, wd, msem.at[1])

    def v_copy(g):
        return pltpu.make_async_copy(
            value_w.at[:, pl.ds(pl.multiple_of(g * GC, GC), GC)], wv.at[g], vsem.at[g]
        )

    def g_copy(g):
        return pltpu.make_async_copy(
            gate_w.at[:, pl.ds(pl.multiple_of(g * GC, GC), GC)], wg.at[g], gsem.at[g]
        )

    d_copy.start()
    for c in x_copies:
        c.start()
    s_copy.start()
    for g in range(G):
        v_copy(g).start()
    for g in range(G):
        g_copy(g).start()

    barrier = pltpu.get_barrier_semaphore()

    def greet(d, _):
        pl.semaphore_signal(
            barrier, inc=1, device_id={"seq": lax.rem(me + d, PEERS)}, device_id_type=MESH
        )
        return 0

    lax.fori_loop(1, PEERS, greet, 0)
    for d in range(1, HEADS_AXIS):
        pl.semaphore_signal(
            barrier, inc=1, device_id={"head": lax.rem(hd + d, HEADS_AXIS)}, device_id_type=MESH
        )

    for g in range(G):
        e512[g] = spread_matrix((128, 512), 4 * g, 128)
        e256[g] = spread_matrix((128, 256), 4 * g, 64)
        for h in range(2):
            eh[h, g] = spread_matrix((128, 128), 2 * (2 * g + h), 64)
    pad[...] = jnp.zeros_like(pad)
    pad[0:1, 0:H] = step_o[...]
    pad[8:9, 0:H] = decay[...]
    pad[16:17, 0:H] = skip[...]
    sq[...] = jnp.zeros_like(sq)

    pl.semaphore_wait(barrier, PEERS - 1 + HEADS_AXIS - 1)

    def halo_copy(dest):
        return pltpu.make_async_remote_copy(
            src_ref=tok.at[:, pl.ds(T - HALO, HALO)],
            dst_ref=x.at[:, pl.ds(0, HALO)],
            send_sem=hsem.at[0],
            recv_sem=hsem.at[1],
            device_id={"seq": dest},
            device_id_type=MESH,
        )

    @pl.when(me < PEERS - 1)
    def _():
        halo_copy(me + 1).start()

    @pl.when(me == 0)
    def _():
        x[:, 0:HALO, :] = jnp.zeros((B, HALO, D), BF16)

    d_copy.wait()
    for c in x_copies:
        c.wait()
    tri = lax.broadcasted_iota(jnp.int32, (L, L), 0) >= lax.broadcasted_iota(jnp.int32, (L, L), 1)
    tri16 = jnp.where(tri, 1.0, 0.0).astype(BF16)
    tri3 = jnp.concatenate([tri16, tri16, tri16], axis=1)
    logsend[...] = jnp.zeros_like(logsend)
    for b in range(B):
        a3f = dot(x[b, HALO:R], wd[...])
        sq[b, :, 0:H] = a3f
        z = sq[b] + pad[0:1]
        step = jnp.maximum(z, 0.0) + jnp.log1p(jnp.exp(-jnp.abs(z)))
        decayed = step * (pad[8:9] * (-LOG2E))
        log_step = jnp.log(step) * LOG2E
        before = jnp.zeros((1, 128), F32)
        for k in range(K):
            part = decayed[k * L : (k + 1) * L]
            hi, mid, low = split3(part)
            stacked = jnp.concatenate([hi, mid, low], axis=0).astype(BF16)
            cum = dot(tri3, stacked)
            last = cum[L - 1 : L]
            source = cum - log_step[k * L : (k + 1) * L]
            a3[b, k] = packed(cum)
            a2w[b, k] = packed(jnp.exp2(last - source))
            a2g[b, k] = packed(jnp.exp2(cum))
            cs_t[b, k] = jnp.transpose(source)[0:32]
            pad[24 + b * K + k : 25 + b * K + k] = jnp.exp2(last)
            pad[32 + b * K + k : 33 + b * K + k] = jnp.exp2(before)
            before = before + last
        logsend[b : b + 1] = before
    sq[...] = jnp.zeros_like(sq)

    def log_copy(dest):
        return pltpu.make_async_remote_copy(
            src_ref=logsend,
            dst_ref=logrecv.at[me],
            send_sem=lsem.at[0],
            recv_sem=lsem.at[1],
            device_id={"seq": dest},
            device_id_type=MESH,
        )

    def send_log(d, _):
        log_copy(lax.rem(me + d, PEERS)).start()
        return 0

    lax.fori_loop(1, PEERS, send_log, 0)
    logrecv[me] = logsend[...]

    rt = packed(pad[24:32])
    rb = packed(pad[32:40])
    rs = packed(pad[16:24])
    for g in range(G):
        rows_t[g] = dot(rt, e256[g])
        rows_b[g] = dot(rb, e256[g])
        rows_s[g] = dot(rs, e256[g])

    s_copy.wait()

    @pl.when(me > 0)
    def _():
        halo_copy(me).wait_recv()

    def convolve(b, raw, taps, offset, j):
        cv[b, j] = raw.astype(BF16).astype(F32)
        total = offset
        for tap in range(TAPS):
            total = total + taps[tap : tap + 1] * cv[b, j, pl.ds(HALO - TAPS + 1 + tap, T), :]
        return silu(total).astype(BF16)

    for b in range(B):
        raw = dot(x[b], ws[...])
        bmap = convolve(b, raw[:, 0:N], state_k[:, 0:N], state_o[:, 0:N], 0)
        cmap = convolve(b, raw[:, N : 2 * N], state_k[:, N : 2 * N], state_o[:, N : 2 * N], 1)
        for k in range(K):
            bk = bmap[k * L : (k + 1) * L]
            ck = cmap[k * L : (k + 1) * L]
            crow[b, k] = ck
            bt = jnp.transpose(bk.astype(F32)).astype(BF16)
            brow_t[b, k] = bt
            sc[b, k] = jnp.where(tri, dot(ck, bt), 0.0)

    def share_copy(g, dest):
        return pltpu.make_async_remote_copy(
            src_ref=sendbuf.at[g, dest],
            dst_ref=recvbuf.at[g, me],
            send_sem=ssem.at[g],
            recv_sem=rsem.at[g],
            device_id={"seq": dest},
            device_id_type=MESH,
        )

    def back_copy(g, dest):
        return pltpu.make_async_remote_copy(
            src_ref=retbuf.at[g, dest],
            dst_ref=retrecv.at[g, me],
            send_sem=tsem.at[g],
            recv_sem=usem.at[g],
            device_id={"seq": dest},
            device_id_type=MESH,
        )

    def value_group(g, _):
        v_copy(g).wait()
        base = pl.multiple_of(g * GC, GC)
        for b in range(B):
            raw = dot(x[b], wv[g])
            for j in range(2):
                at = pl.ds(pl.multiple_of(base + j * 128, 128), 128)
                vbuf[g, b, :, j * 128 : (j + 1) * 128] = convolve(
                    b, raw[:, j * 128 : (j + 1) * 128], value_k[:, at], value_o[:, at], j
                )
            state = None
            for k in range(K):
                scale = dot(a2w[b, k], e256[g])
                vk = vbuf[g, b, k * L : (k + 1) * L].astype(F32)
                made = dot(brow_t[b, k], (vk * scale).astype(BF16))
                if state is None:
                    state = made
                else:
                    local[g, b, k - 1] = state
                    state = state * rows_t[g, b * K + k : b * K + k + 1] + made
            state = state.astype(BF16)
            for h in range(2):
                first = (b * 2 + h) * 8
                sendbuf[g, first : first + 8] = state[:, h * 128 : (h + 1) * 128].reshape(8, 16, 128)

        def send(d, _):
            share_copy(g, lax.rem(me + d, PEERS)).start()
            return 0

        lax.fori_loop(1, PEERS, send, 0)
        recvbuf[g, me] = sendbuf[g, me]
        return 0

    lax.fori_loop(0, G, value_group, 0)

    def all_logs():
        return pltpu.make_async_remote_copy(
            src_ref=logrecv.at[pl.ds(0, PEERS - 1)],
            dst_ref=logrecv.at[pl.ds(0, PEERS - 1)],
            send_sem=lsem.at[0],
            recv_sem=lsem.at[1],
            device_id={"seq": me},
            device_id_type=MESH,
        )

    all_logs().wait_recv()
    my_batch = me // 16
    my_half = lax.rem(me // 8, 2)
    logs = logrecv[:, pl.ds(my_batch, 1), :].reshape(PEERS, 128)
    through = packed(jnp.exp2(logs))
    for g in range(G):
        fac[g] = dot(through, eh[my_half, g])

    first_half = lax.broadcasted_iota(jnp.int32, (L, 128), 1) < 64

    def bulk(buf, g, send, recv):
        return pltpu.make_async_remote_copy(
            src_ref=buf.at[g, pl.ds(0, PEERS - 1)],
            dst_ref=buf.at[g, pl.ds(0, PEERS - 1)],
            send_sem=send.at[g],
            recv_sem=recv.at[g],
            device_id={"seq": me},
            device_id_type=MESH,
        )

    def gate_group(g, _):
        g_copy(g).wait()
        bulk(recvbuf, g, ssem, rsem).wait_recv()
        chain = jnp.zeros((16, 128), F32)
        for j in range(PEERS):
            retbuf[g, j] = chain.astype(BF16)
            chain = chain * fac[g, j : j + 1] + recvbuf[g, j].astype(F32)

        def send(d, _):
            back_copy(g, lax.rem(me + d, PEERS)).start()
            return 0

        lax.fori_loop(1, PEERS, send, 0)
        retrecv[g, me] = retbuf[g, me]
        for b in range(B):
            gbuf[g, b] = dot(x[b, HALO:R], wg[g]).astype(BF16)
            for k in range(K):
                rows = slice(k * L, (k + 1) * L)
                target = dot(a3[b, k], e512[g])
                for p in range(2):
                    lanes = slice(p * 128, (p + 1) * 128)
                    mixes = []
                    for q in range(2):
                        n = 2 * p + q
                        spread = target[:, n * 128 : (n + 1) * 128] - cs_t[b, k, pl.ds(4 * g + n, 1), :]
                        mixes.append((jnp.exp2(jnp.minimum(spread, 100.0)) * sc[b, k]).astype(BF16))
                    mix = jnp.concatenate(mixes, axis=1)
                    v = vbuf[g, b, rows, lanes].astype(F32)
                    two = jnp.concatenate(
                        [jnp.where(first_half, v, 0.0), jnp.where(first_half, 0.0, v)], axis=0
                    ).astype(BF16)
                    mixbuf[g, b, rows, lanes] = dot(mix, two) + rows_s[g, 0:1, lanes] * v
        return 0

    lax.fori_loop(0, G, gate_group, 0)

    def carry_group(g, _):
        bulk(retrecv, g, tsem, usem).wait_recv()
        for b in range(B):
            halves = [
                retrecv[g, (b * 2 + h) * 8 : (b * 2 + h) * 8 + 8].reshape(128, 128) for h in range(2)
            ]
            entering = jnp.concatenate(halves, axis=1).astype(F32)
            for k in range(K):
                rows = slice(k * L, (k + 1) * L)
                if k == 0:
                    state = entering
                else:
                    state = local[g, b, k - 1] + entering * rows_b[g, b * K + k : b * K + k + 1]
                carried = dot(crow[b, k], state.astype(BF16))
                inside = dot(a2g[b, k], e256[g])
                mixture = mixbuf[g, b, rows] + inside * carried
                gated = mixture * silu(gbuf[g, b, rows].astype(F32))
                mixbuf[g, b, rows] = gated
                square = gated * gated
                sq[b, rows] = sq[b, rows] + square[:, 0:128] + square[:, 128:256]
        return 0

    lax.fori_loop(0, G, carry_group, 0)

    ones = jnp.ones((8, 256), BF16)
    for b in range(B):
        hi, mid, _ = split3(sq[b])
        terms = jnp.concatenate([hi, mid], axis=1).astype(BF16)
        ssend[b] = lax.dot_general(ones, terms, (((1,), (1,)), ((), ())), preferred_element_type=F32)

    def square_copy(d):
        return pltpu.make_async_remote_copy(
            src_ref=ssend,
            dst_ref=srecv.at[hd],
            send_sem=qsem.at[0],
            recv_sem=qsem.at[1],
            device_id={"head": lax.rem(hd + d, HEADS_AXIS)},
            device_id_type=MESH,
        )

    for d in range(1, HEADS_AXIS):
        square_copy(d).start()
    srecv[hd] = ssend[...]
    pltpu.make_async_remote_copy(
        src_ref=srecv.at[pl.ds(0, HEADS_AXIS - 1)],
        dst_ref=srecv.at[pl.ds(0, HEADS_AXIS - 1)],
        send_sem=qsem.at[0],
        recv_sem=qsem.at[1],
        device_id={"head": hd},
        device_id_type=MESH,
    ).wait_recv()
    eighth = jnp.full((16, 128), 0.125, BF16)
    for b in range(B):
        total = srecv[0, b] + srecv[1, b] + srecv[2, b] + srecv[3, b]
        inverse = lax.rsqrt(total / INNER + EPS)
        hi, mid, _ = split3(inverse)
        terms = jnp.concatenate([hi, mid], axis=0).astype(BF16)
        sq[b] = lax.dot_general(terms, eighth, (((0,), (0,)), ((), ())), preferred_element_type=F32)

    def out_copy(g):
        return pltpu.make_async_copy(
            obuf.at[g], out.at[:, :, pl.ds(pl.multiple_of(g * GC, GC), GC)], osem.at[g]
        )

    def final_group(g, _):
        base = pl.multiple_of(g * GC, GC)
        for b in range(B):
            for j in range(2):
                lanes = slice(j * 128, (j + 1) * 128)
                at = pl.ds(pl.multiple_of(base + j * 128, 128), 128)
                obuf[g, b, :, lanes] = (mixbuf[g, b, :, lanes] * sq[b] * gain[:, at]).astype(BF16)
        out_copy(g).start()
        return 0

    lax.fori_loop(0, G, final_group, 0)

    def finish(g, _):
        out_copy(g).wait()
        bulk(sendbuf, g, ssem, rsem).wait_send()
        bulk(retbuf, g, tsem, usem).wait_send()
        return 0

    lax.fori_loop(0, G, finish, 0)
    all_logs().wait_send()
    pltpu.make_async_remote_copy(
        src_ref=srecv.at[pl.ds(0, HEADS_AXIS - 1)],
        dst_ref=srecv.at[pl.ds(0, HEADS_AXIS - 1)],
        send_sem=qsem.at[0],
        recv_sem=qsem.at[1],
        device_id={"head": hd},
        device_id_type=MESH,
    ).wait_send()

    @pl.when(me < PEERS - 1)
    def _():
        halo_copy(me + 1).wait_send()


def local_program(
    tokens, gate_weight, value_weight, state_weight, step_weight, value_kernel, value_offset,
    state_kernel, state_offset, step_offset, decay_rate, skip_gain, norm_gain,
):
    anywhere = pl.BlockSpec(memory_space=pl.ANY)
    inside = pl.BlockSpec(memory_space=pltpu.VMEM)
    vm = pltpu.VMEM
    dma = pltpu.SemaphoreType.DMA
    return pl.pallas_call(
        body,
        out_shape=jax.ShapeDtypeStruct((B, T, C), BF16),
        in_specs=[anywhere] * 5 + [inside] * 8,
        out_specs=anywhere,
        scratch_shapes=[
            vm((B, R, D), BF16),
            vm((G, D, GC), BF16),
            vm((G, D, GC), BF16),
            vm((D, 2 * N), BF16),
            vm((D, H), BF16),
            vm((B, 2, R, 128), F32),
            vm((G, B, T, GC), BF16),
            vm((G, B, T, GC), BF16),
            vm((G, B, T, GC), F32),
            vm((B, K, N, L), BF16),
            vm((B, K, L, N), BF16),
            vm((B, K, L, L), F32),
            vm((B, K, L, 128), BF16),
            vm((B, K, L, 128), BF16),
            vm((B, K, L, 128), BF16),
            vm((B, K, 32, L), F32),
            vm((G, 128, 512), BF16),
            vm((G, 128, 256), BF16),
            vm((2, G, 128, 128), BF16),
            vm((G, 8, GC), F32),
            vm((G, 8, GC), F32),
            vm((G, 8, GC), F32),
            vm((40, 128), F32),
            vm((G, B, K - 1, N, GC), F32),
            vm((G, PEERS, 16, 128), BF16),
            vm((G, PEERS, 16, 128), BF16),
            vm((G, PEERS, 16, 128), BF16),
            vm((G, PEERS, 16, 128), BF16),
            vm((8, 128), F32),
            vm((PEERS, 8, 128), F32),
            vm((G, PEERS, 128), F32),
            vm((B, T, 128), F32),
            vm((B, 8, T), F32),
            vm((HEADS_AXIS, B, 8, T), F32),
            vm((G, B, T, GC), BF16),
            dma((B,)), dma((G,)), dma((G,)), dma((2,)), dma((G,)), dma((2,)),
            dma((G,)), dma((G,)), dma((G,)), dma((G,)), dma((2,)), dma((2,)),
        ],
        compiler_params=pltpu.CompilerParams(
            collective_id=0, has_side_effects=True, vmem_limit_bytes=64 * 1024 * 1024 - 65536
        ),
        name="mixer",
    )(
        tokens, gate_weight, value_weight, state_weight, step_weight, value_kernel,
        value_offset.reshape(1, C), state_kernel, state_offset.reshape(1, 2 * N),
        step_offset.reshape(1, H), decay_rate.reshape(1, H), skip_gain.reshape(1, H),
        norm_gain.reshape(1, C),
    )


def solution(mesh):
    return jax.shard_map(
        local_program,
        mesh=mesh,
        in_specs=(
            P(None, "seq", None),
            P(None, "head"),
            P(None, "head"),
            P(),
            P(None, "head"),
            P(None, "head"),
            P("head"),
            P(),
            P(),
            P("head"),
            P("head"),
            P("head"),
            P("head"),
        ),
        out_specs=P(None, "seq", "head"),
        check_vma=False,
    )
```

```python
import functools

import jax
import jax.numpy as jnp
from jax import lax
from jax.experimental import pallas as pl
from jax.experimental.pallas import tpu as pltpu
from jax.sharding import PartitionSpec as P

MESH = pl.DeviceIdType.MESH
F32 = jnp.float32
BF16 = jnp.bfloat16

EPS = 1e-05
LOG2E = 1.4426950408889634
B = 2
T = 512
D = 2560
C = 1280
H = 20
N = 128
L = 128
K = T // L
GC = 256
G = C // GC
HALO = 16
R = T + HALO
TAPS = 4
PEERS = 32
HEADS_AXIS = 4
INNER = 5120


def dot(a, b):
    return jnp.dot(a, b, preferred_element_type=F32)


def split3(x):
    hi = x.astype(BF16).astype(F32)
    rest = x - hi
    mid = rest.astype(BF16).astype(F32)
    return hi, mid, rest - mid


def packed(x):
    lane = lax.broadcasted_iota(jnp.int32, x.shape, 1)
    hi, mid, low = split3(jnp.where(lane < H, x, 0.0))
    return (hi + pltpu.roll(mid, 32, 1) + pltpu.roll(low, 64, 1)).astype(BF16)


def silu(x):
    half = 0.5 * x
    return half * jnp.tanh(half) + half


def spread_matrix(shape, first_head, width):
    row = lax.broadcasted_iota(jnp.int32, shape, 0)
    col = lax.broadcasted_iota(jnp.int32, shape, 1)
    hit = (row & 31) == (first_head + col // width)
    return jnp.where(hit & (row < 96), 1.0, 0.0).astype(BF16)


def body(
    tok, gate_w, value_w, state_w, step_w,
    value_k, value_o, state_k, state_o, step_o, decay, skip,
    mixbuf, inverse_out,
    x, wv, wg, ws, wd, cv, cm, vbuf, gbuf, brow_t, crow, sc, cums, closing, a2g, cs_t,
    e256, eh, rows_t, rows_b, rows_s, pad, local, sendbuf, recvbuf, retbuf, retrecv,
    logsend, logrecv, fac, sq, ssend, srecv,
    xsem, vsem, gsem, msem, hsem, ssem, rsem, tsem, usem, lsem, qsem,
):
    me = lax.axis_index("seq")
    hd = lax.axis_index("head")

    x_copies = [
        pltpu.make_async_copy(tok.at[b], x.at[b, pl.ds(HALO, T)], xsem.at[b]) for b in range(B)
    ]
    s_copy = pltpu.make_async_copy(state_w, ws, msem.at[0])
    d_copy = pltpu.make_async_copy(step_w, wd, msem.at[1])

    def v_copy(g):
        return pltpu.make_async_copy(
            value_w.at[:, pl.ds(pl.multiple_of(g * GC, GC), GC)], wv.at[g], vsem.at[g]
        )

    def g_copy(g):
        return pltpu.make_async_copy(
            gate_w.at[:, pl.ds(pl.multiple_of(g * GC, GC), GC)], wg.at[g], gsem.at[g]
        )

    d_copy.start()
    for c in x_copies:
        c.start()
    s_copy.start()
    for g in range(G):
        v_copy(g).start()
    for g in range(G):
        g_copy(g).start()

    barrier = pltpu.get_barrier_semaphore()

    def greet(d, _):
        pl.semaphore_signal(
            barrier, inc=1, device_id={"seq": lax.rem(me + d, PEERS)}, device_id_type=MESH
        )
        return 0

    lax.fori_loop(1, PEERS, greet, 0)
    for d in range(1, HEADS_AXIS):
        pl.semaphore_signal(
            barrier, inc=1, device_id={"head": lax.rem(hd + d, HEADS_AXIS)}, device_id_type=MESH
        )

    for g in range(G):
        e256[g] = spread_matrix((128, 256), 4 * g, 64)
        for h in range(2):
            eh[h, g] = spread_matrix((128, 128), 2 * (2 * g + h), 64)
    pad[...] = jnp.zeros_like(pad)
    pad[0:1, 0:H] = step_o[...]
    pad[8:9, 0:H] = decay[...]
    pad[16:17, 0:H] = skip[...]
    sq[...] = jnp.zeros_like(sq)

    def halo_copy(dest):
        return pltpu.make_async_remote_copy(
            src_ref=tok.at[:, pl.ds(T - HALO, HALO)],
            dst_ref=x.at[:, pl.ds(0, HALO)],
            send_sem=hsem.at[0],
            recv_sem=hsem.at[1],
            device_id={"seq": dest},
            device_id_type=MESH,
        )

    d_copy.wait()
    for c in x_copies:
        c.wait()
    step_raw = [
        lax.dot_general(
            x[b, HALO:R], wd[...], (((1,), (1,)), ((), ())), preferred_element_type=F32
        )
        for b in range(B)
    ]
    tri = lax.broadcasted_iota(jnp.int32, (L, L), 0) >= lax.broadcasted_iota(jnp.int32, (L, L), 1)
    tri16 = jnp.where(tri, 1.0, 0.0).astype(BF16)
    tri3 = jnp.concatenate([tri16, tri16, tri16], axis=1)
    logsend[...] = jnp.zeros_like(logsend)
    for b in range(B):
        a3f = step_raw[b]
        sq[b, :, 0:H] = a3f
        z = sq[b] + pad[0:1]
        step = jnp.maximum(z, 0.0) + jnp.log1p(jnp.exp(-jnp.abs(z)))
        decayed = step * (pad[8:9] * (-LOG2E))
        log_step = jnp.log(step) * LOG2E
        before = jnp.zeros((1, 128), F32)
        for k in range(K):
            part = decayed[k * L : (k + 1) * L]
            hi, mid, low = split3(part)
            stacked = jnp.concatenate([hi, mid, low], axis=0).astype(BF16)
            cum = dot(tri3, stacked)
            last = cum[L - 1 : L]
            source = cum - log_step[k * L : (k + 1) * L]
            cums[b, k] = cum
            closing[b, k] = jnp.exp2(last - source)
            a2g[b, k] = packed(jnp.exp2(cum))
            cs_t[b, k] = jnp.transpose(source)[0:32]
            pad[24 + b * K + k : 25 + b * K + k] = jnp.exp2(last)
            pad[32 + b * K + k : 33 + b * K + k] = jnp.exp2(before)
            before = before + last
        logsend[b : b + 1] = before
    sq[...] = jnp.zeros_like(sq)

    def log_copy(dest):
        return pltpu.make_async_remote_copy(
            src_ref=logsend,
            dst_ref=logrecv.at[me],
            send_sem=lsem.at[0],
            recv_sem=lsem.at[1],
            device_id={"seq": dest},
            device_id_type=MESH,
        )

    pl.semaphore_wait(barrier, PEERS - 1 + HEADS_AXIS - 1)


    @pl.when(me < PEERS - 1)
    def _():
        halo_copy(me + 1).start()

    @pl.when(me == 0)
    def _():
        x[:, 0:HALO, :] = jnp.zeros((B, HALO, D), BF16)

    def send_log(d, _):
        log_copy(lax.rem(me + d, PEERS)).start()
        return 0

    lax.fori_loop(1, PEERS, send_log, 0)
    logrecv[me] = logsend[...]

    rt = packed(pad[24:32])
    rb = packed(pad[32:40])
    rs = packed(pad[16:24])
    for g in range(G):
        rows_t[g] = dot(rt, e256[g])
        rows_b[g] = dot(rb, e256[g])
        rows_s[g] = dot(rs, e256[g])

    s_copy.wait()

    @pl.when(me > 0)
    def _():
        halo_copy(me).wait_recv()

    def share_copy(g, dest):
        return pltpu.make_async_remote_copy(
            src_ref=sendbuf.at[g, dest],
            dst_ref=recvbuf.at[g, me],
            send_sem=ssem.at[g],
            recv_sem=rsem.at[g],
            device_id={"seq": dest},
            device_id_type=MESH,
        )

    def back_copy(g, dest):
        return pltpu.make_async_remote_copy(
            src_ref=retbuf.at[g, dest],
            dst_ref=retrecv.at[g, me],
            send_sem=tsem.at[g],
            recv_sem=usem.at[g],
            device_id={"seq": dest},
            device_id_type=MESH,
        )

    first_half = lax.broadcasted_iota(jnp.int32, (L, 128), 1) < 64

    def to_front(heads, g):
        return pltpu.roll(heads, lax.rem(128 - 4 * g, 128), 1)

    def column(heads, n):
        return jnp.broadcast_to(heads[:, n : n + 1], (L, 128))

    def value_dot(g, b):
        for first in range(0, R, R // 2):
            raw = dot(x[b, first : first + R // 2], wv[g]).astype(BF16).astype(F32)
            for j in range(2):
                cv[b, j, first : first + R // 2] = raw[:, j * 128 : (j + 1) * 128]

    def value_conv(g, b):
        for j in range(2):
            at = pl.ds(pl.multiple_of(g * GC + j * 128, 128), 128)
            vbuf[g, b, :, j * 128 : (j + 1) * 128] = convolve(
                cv, b, value_k[:, at], value_o[pl.ds(2 * g + j, 1), :], j
            )

    def value_state(g, b):
        state = None
        for k in range(K):
            near = to_front(closing[b, k], g)
            scale = jnp.concatenate(
                [jnp.where(first_half, column(near, 2 * j), column(near, 2 * j + 1)) for j in range(2)],
                axis=1,
            )
            vk = vbuf[g, b, k * L : (k + 1) * L].astype(F32)
            made = dot(brow_t[b, k], (vk * scale).astype(BF16))
            if state is None:
                state = made
            else:
                local[g, b, k - 1] = state
                state = state * rows_t[g, b * K + k : b * K + k + 1] + made
        state = state.astype(BF16)
        for h in range(2):
            first = (b * 2 + h) * 8
            sendbuf[g, first : first + 8] = state[:, h * 128 : (h + 1) * 128].reshape(8, 16, 128)

    def send_shares(g):
        def send(d, _):
            share_copy(g, lax.rem(me + d, PEERS)).start()
            return 0

        lax.fori_loop(1, PEERS, send, 0)
        recvbuf[g, me] = sendbuf[g, me]

    def convolve(raw, b, taps, offset, j):
        total = offset
        for tap in range(TAPS):
            total = total + taps[tap : tap + 1] * raw[b, j, pl.ds(HALO - TAPS + 1 + tap, T), :]
        return silu(total).astype(BF16)

    for b in range(B):
        for first in range(0, R, R // 2):
            raw = dot(x[b, first : first + R // 2], ws[...]).astype(BF16).astype(F32)
            for j in range(2):
                cm[b, j, first : first + R // 2] = raw[:, j * 128 : (j + 1) * 128]
    v_copy(0).wait()
    for b in range(B):
        value_dot(0, b)
        bmap = convolve(cm, b, state_k[:, 0:N], state_o[0:1], 0)
        cmap = convolve(cm, b, state_k[:, N : 2 * N], state_o[1:2], 1)
        for k in range(K):
            bk = bmap[k * L : (k + 1) * L]
            ck = cmap[k * L : (k + 1) * L]
            crow[b, k] = ck
            bt = jnp.transpose(bk.astype(F32)).astype(BF16)
            brow_t[b, k] = bt
            sc[b, k] = jnp.where(tri, dot(ck, bt), 0.0)

    def value_group(g, _):
        v_copy(g).wait()
        for b in range(B):
            value_conv(g - 1, b)
        for b in range(B):
            value_dot(g, b)
            value_state(g - 1, b)
        send_shares(g - 1)
        return 0

    lax.fori_loop(1, G, value_group, 0)

    def all_logs():
        return pltpu.make_async_remote_copy(
            src_ref=logrecv.at[pl.ds(0, PEERS - 1)],
            dst_ref=logrecv.at[pl.ds(0, PEERS - 1)],
            send_sem=lsem.at[0],
            recv_sem=lsem.at[1],
            device_id={"seq": me},
            device_id_type=MESH,
        )


    def bulk(buf, g, send, recv):
        return pltpu.make_async_remote_copy(
            src_ref=buf.at[g, pl.ds(0, PEERS - 1)],
            dst_ref=buf.at[g, pl.ds(0, PEERS - 1)],
            send_sem=send.at[g],
            recv_sem=recv.at[g],
            device_id={"seq": me},
            device_id_type=MESH,
        )

    def gate_dot(g, b):
        for first in range(0, T, T // 2):
            rows = slice(first, first + T // 2)
            gbuf[g, b, rows] = dot(x[b, HALO + first : HALO + first + T // 2], wg[g]).astype(BF16)

    def within(g, b):
        for k in range(K):
            rows = slice(k * L, (k + 1) * L)
            near = to_front(cums[b, k], g)
            for p in range(2):
                lanes = slice(p * 128, (p + 1) * 128)
                mixes = []
                for q in range(2):
                    n = 2 * p + q
                    spread = column(near, n) - cs_t[b, k, pl.ds(4 * g + n, 1), :]
                    mixes.append((jnp.exp2(jnp.minimum(spread, 100.0)) * sc[b, k]).astype(BF16))
                mix = jnp.concatenate(mixes, axis=1)
                v = vbuf[g, b, rows, lanes].astype(F32)
                two = jnp.concatenate(
                    [jnp.where(first_half, v, 0.0), jnp.where(first_half, 0.0, v)], axis=0
                ).astype(BF16)
                mixbuf[g, b, rows, lanes] = dot(mix, two) + rows_s[g, 0:1, lanes] * v

    def chain_share(g):
        bulk(recvbuf, g, ssem, rsem).wait_recv()
        chain = jnp.zeros((16, 128), F32)
        for j in range(PEERS):
            retbuf[g, j] = chain.astype(BF16)
            chain = chain * fac[g, j : j + 1] + recvbuf[g, j].astype(F32)

        def send(d, _):
            back_copy(g, lax.rem(me + d, PEERS)).start()
            return 0

        lax.fori_loop(1, PEERS, send, 0)
        retrecv[g, me] = retbuf[g, me]

    g_copy(0).wait()
    for b in range(B):
        value_conv(G - 1, b)
    for b in range(B):
        gate_dot(0, b)
        value_state(G - 1, b)
    send_shares(G - 1)

    all_logs().wait_recv()
    my_batch = me // 16
    my_half = lax.rem(me // 8, 2)
    logs = logrecv[:, pl.ds(my_batch, 1), :].reshape(PEERS, 128)
    through = packed(jnp.exp2(logs))
    for g in range(G):
        fac[g] = dot(through, eh[my_half, g])

    def gate_group(g, _):
        g_copy(g).wait()
        for b in range(B):
            gate_dot(g, b)
            within(g - 1, b)
        return 0

    lax.fori_loop(1, G, gate_group, 0)

    def chain_group(g, _):
        chain_share(g)
        return 0

    lax.fori_loop(0, G, chain_group, 0)
    for b in range(B):
        within(G - 1, b)

    def carry_group(g, _):
        bulk(retrecv, g, tsem, usem).wait_recv()
        for b in range(B):
            halves = [
                retrecv[g, (b * 2 + h) * 8 : (b * 2 + h) * 8 + 8].reshape(128, 128) for h in range(2)
            ]
            entering = jnp.concatenate(halves, axis=1).astype(F32)
            for k in range(K):
                rows = slice(k * L, (k + 1) * L)
                if k == 0:
                    state = entering
                else:
                    state = local[g, b, k - 1] + entering * rows_b[g, b * K + k : b * K + k + 1]
                carried = dot(crow[b, k], state.astype(BF16))
                inside = dot(a2g[b, k], e256[g])
                mixture = mixbuf[g, b, rows] + inside * carried
                gated = mixture * silu(gbuf[g, b, rows].astype(F32))
                mixbuf[g, b, rows] = gated
                square = gated * gated
                sq[b, rows] = sq[b, rows] + square[:, 0:128] + square[:, 128:256]
        return 0

    lax.fori_loop(0, G, carry_group, 0)

    ones = jnp.ones((8, 256), BF16)
    for b in range(B):
        hi, mid, _ = split3(sq[b])
        terms = jnp.concatenate([hi, mid], axis=1).astype(BF16)
        ssend[b] = lax.dot_general(ones, terms, (((1,), (1,)), ((), ())), preferred_element_type=F32)

    def square_copy(d):
        return pltpu.make_async_remote_copy(
            src_ref=ssend,
            dst_ref=srecv.at[hd],
            send_sem=qsem.at[0],
            recv_sem=qsem.at[1],
            device_id={"head": lax.rem(hd + d, HEADS_AXIS)},
            device_id_type=MESH,
        )

    for d in range(1, HEADS_AXIS):
        square_copy(d).start()
    srecv[hd] = ssend[...]
    pltpu.make_async_remote_copy(
        src_ref=srecv.at[pl.ds(0, HEADS_AXIS - 1)],
        dst_ref=srecv.at[pl.ds(0, HEADS_AXIS - 1)],
        send_sem=qsem.at[0],
        recv_sem=qsem.at[1],
        device_id={"head": hd},
        device_id_type=MESH,
    ).wait_recv()
    eighth = jnp.full((16, 128), 0.125, BF16)
    for b in range(B):
        total = srecv[0, b] + srecv[1, b] + srecv[2, b] + srecv[3, b]
        inverse = lax.rsqrt(total / INNER + EPS)
        hi, mid, _ = split3(inverse)
        terms = jnp.concatenate([hi, mid], axis=0).astype(BF16)
        inverse_out[b] = lax.dot_general(terms, eighth, (((0,), (0,)), ((), ())), preferred_element_type=F32)

    def finish(g, _):
        bulk(sendbuf, g, ssem, rsem).wait_send()
        bulk(retbuf, g, tsem, usem).wait_send()
        return 0

    lax.fori_loop(0, G, finish, 0)
    all_logs().wait_send()
    pltpu.make_async_remote_copy(
        src_ref=srecv.at[pl.ds(0, HEADS_AXIS - 1)],
        dst_ref=srecv.at[pl.ds(0, HEADS_AXIS - 1)],
        send_sem=qsem.at[0],
        recv_sem=qsem.at[1],
        device_id={"head": hd},
        device_id_type=MESH,
    ).wait_send()

    @pl.when(me < PEERS - 1)
    def _():
        halo_copy(me + 1).wait_send()


def scale(gated, inverse, gain, out, obuf, sem):
    copies = []
    for g in range(G):
        for b in range(B):
            for j in range(2):
                lanes = slice(j * 128, (j + 1) * 128)
                obuf[g, b, :, lanes] = (
                    gated[g, b, :, lanes] * inverse[b] * gain[2 * g + j : 2 * g + j + 1]
                ).astype(BF16)
            copies.append(
                pltpu.make_async_copy(
                    obuf.at[g, b], out.at[b, :, pl.ds(g * GC, GC)], sem.at[g, b]
                )
            )
            copies[-1].start()
    for c in copies:
        c.wait()


def local_program(
    tokens, gate_weight, value_weight, state_weight, step_weight, value_kernel, value_offset,
    state_kernel, state_offset, step_offset, decay_rate, skip_gain, norm_gain,
):
    anywhere = pl.BlockSpec(memory_space=pl.ANY)
    inside = pl.BlockSpec(memory_space=pltpu.VMEM)
    vm = pltpu.VMEM
    dma = pltpu.SemaphoreType.DMA
    gated, inverse = pl.pallas_call(
        body,
        out_shape=(vm((G, B, T, GC), F32), vm((B, T, 128), F32)),
        in_specs=[anywhere] * 5 + [inside] * 7,
        out_specs=(inside, inside),
        scratch_shapes=[
            vm((B, R, D), BF16),
            vm((G, D, GC), BF16),
            vm((G, D, GC), BF16),
            vm((D, 2 * N), BF16),
            vm((H, D), BF16),
            vm((B, 2, R, 128), F32),
            vm((B, 2, R, 128), F32),
            vm((G, B, T, GC), BF16),
            vm((G, B, T, GC), BF16),
            vm((B, K, N, L), BF16),
            vm((B, K, L, N), BF16),
            vm((B, K, L, L), F32),
            vm((B, K, L, 128), F32),
            vm((B, K, L, 128), F32),
            vm((B, K, L, 128), BF16),
            vm((B, K, 32, L), F32),
            vm((G, 128, 256), BF16),
            vm((2, G, 128, 128), BF16),
            vm((G, 8, GC), F32),
            vm((G, 8, GC), F32),
            vm((G, 8, GC), F32),
            vm((40, 128), F32),
            vm((G, B, K - 1, N, GC), F32),
            vm((G, PEERS, 16, 128), BF16),
            vm((G, PEERS, 16, 128), BF16),
            vm((G, PEERS, 16, 128), BF16),
            vm((G, PEERS, 16, 128), BF16),
            vm((8, 128), F32),
            vm((PEERS, 8, 128), F32),
            vm((G, PEERS, 128), F32),
            vm((B, T, 128), F32),
            vm((B, 8, T), F32),
            vm((HEADS_AXIS, B, 8, T), F32),
            dma((B,)), dma((G,)), dma((G,)), dma((2,)), dma((2,)),
            dma((G,)), dma((G,)), dma((G,)), dma((G,)), dma((2,)), dma((2,)),
        ],
        compiler_params=pltpu.CompilerParams(
            collective_id=0, has_side_effects=True, vmem_limit_bytes=50 * 1024 * 1024
        ),
        name="mixer",
    )(
        tokens, gate_weight, value_weight, state_weight, step_weight.T, value_kernel,
        value_offset.reshape(C // 128, 128), state_kernel, state_offset.reshape(2, N),
        step_offset.reshape(1, H), decay_rate.reshape(1, H), skip_gain.reshape(1, H),
    )
    return pl.pallas_call(
        scale,
        out_shape=jax.ShapeDtypeStruct((B, T, C), BF16),
        in_specs=[inside] * 3,
        out_specs=anywhere,
        scratch_shapes=[vm((G, B, T, GC), BF16), dma((G, B))],
        compiler_params=pltpu.CompilerParams(vmem_limit_bytes=8 * 1024 * 1024),
        name="scale",
    )(gated, inverse, norm_gain.reshape(C // 128, 128))


def solution(mesh):
    return jax.shard_map(
        local_program,
        mesh=mesh,
        in_specs=(
            P(None, "seq", None),
            P(None, "head"),
            P(None, "head"),
            P(),
            P(None, "head"),
            P(None, "head"),
            P("head"),
            P(),
            P(),
            P("head"),
            P("head"),
            P("head"),
            P("head"),
        ),
        out_specs=P(None, "seq", "head"),
        check_vma=False,
    )
```

```python
import functools

import jax
import jax.numpy as jnp
from jax import lax
from jax.experimental import pallas as pl
from jax.experimental.pallas import tpu as pltpu
from jax.sharding import PartitionSpec as P

MESH = pl.DeviceIdType.MESH
F32 = jnp.float32
BF16 = jnp.bfloat16

EPS = 1e-05
LOG2E = 1.4426950408889634
B = 2
T = 512
D = 2560
C = 1280
H = 20
N = 128
L = 128
K = T // L
GC = 256
G = C // GC
HALO = 16
R = T + HALO
TAPS = 4
PEERS = 32
HEADS_AXIS = 4
INNER = 5120


def dot(a, b):
    return jnp.dot(a, b, preferred_element_type=F32)


def split3(x):
    hi = x.astype(BF16).astype(F32)
    rest = x - hi
    mid = rest.astype(BF16).astype(F32)
    return hi, mid, rest - mid


def packed(x):
    lane = lax.broadcasted_iota(jnp.int32, x.shape, 1)
    hi, mid, low = split3(jnp.where(lane < H, x, 0.0))
    return (hi + pltpu.roll(mid, 32, 1) + pltpu.roll(low, 64, 1)).astype(BF16)


def silu(x):
    half = 0.5 * x
    return half * jnp.tanh(half) + half


def spread_matrix(shape, first_head, width):
    row = lax.broadcasted_iota(jnp.int32, shape, 0)
    col = lax.broadcasted_iota(jnp.int32, shape, 1)
    hit = (row & 31) == (first_head + col // width)
    return jnp.where(hit & (row < 96), 1.0, 0.0).astype(BF16)


def body(
    tok, gate_w, value_w, state_w, step_w,
    value_k_in, value_o_in, state_k_in, state_o_in, step_o_in, decay_in, skip_in,
    mixbuf, inverse_out,
    value_k, value_o, state_k, state_o, step_o, decay, skip,
    x, wv, wg, ws, wd, cv, cm, vbuf, gbuf, brow_t, crow, sc, cums, closing, a2g, cs_t,
    e256, eh, rows_t, rows_b, rows_s, pad, local, sendbuf, recvbuf, retbuf, retrecv,
    logsend, logrecv, fac, sq, ssend, srecv,
    xsem, vsem, gsem, msem, psem, hsem, ssem, rsem, tsem, usem, lsem, qsem,
):
    me = lax.axis_index("seq")
    hd = lax.axis_index("head")

    x_copies = [
        pltpu.make_async_copy(tok.at[b], x.at[b, pl.ds(HALO, T)], xsem.at[b]) for b in range(B)
    ]
    s_copy = pltpu.make_async_copy(state_w, ws, msem.at[0])
    d_copy = pltpu.make_async_copy(step_w, wd, msem.at[1])

    def v_copy(g):
        return pltpu.make_async_copy(
            value_w.at[:, pl.ds(pl.multiple_of(g * GC, GC), GC)], wv.at[g], vsem.at[g]
        )

    def g_copy(g):
        return pltpu.make_async_copy(
            gate_w.at[:, pl.ds(pl.multiple_of(g * GC, GC), GC)], wg.at[g], gsem.at[g]
        )

    small = [
        pltpu.make_async_copy(src, dst, psem.at[i])
        for i, (src, dst) in enumerate(
            (
                (step_o_in, step_o), (decay_in, decay), (skip_in, skip), (state_k_in, state_k),
                (state_o_in, state_o), (value_k_in, value_k), (value_o_in, value_o),
            )
        )
    ]
    d_copy.start()
    for c in x_copies:
        c.start()
    for c in small:
        c.start()
    s_copy.start()
    v_copy(0).start()

    barrier = pltpu.get_barrier_semaphore()

    def greet(d, _):
        pl.semaphore_signal(
            barrier, inc=1, device_id={"seq": lax.rem(me + d, PEERS)}, device_id_type=MESH
        )
        return 0

    lax.fori_loop(1, PEERS, greet, 0)
    for d in range(1, HEADS_AXIS):
        pl.semaphore_signal(
            barrier, inc=1, device_id={"head": lax.rem(hd + d, HEADS_AXIS)}, device_id_type=MESH
        )

    for g in range(G):
        e256[g] = spread_matrix((128, 256), 4 * g, 64)
        for h in range(2):
            eh[h, g] = spread_matrix((128, 128), 2 * (2 * g + h), 64)
    pad[...] = jnp.zeros_like(pad)
    sq[...] = jnp.zeros_like(sq)
    logsend[...] = jnp.zeros_like(logsend)

    def halo_copy(dest):
        return pltpu.make_async_remote_copy(
            src_ref=tok.at[:, pl.ds(T - HALO, HALO)],
            dst_ref=x.at[:, pl.ds(0, HALO)],
            send_sem=hsem.at[0],
            recv_sem=hsem.at[1],
            device_id={"seq": dest},
            device_id_type=MESH,
        )

    d_copy.wait()
    for b in range(B):
        x_copies[b].wait()
        for first in range(0, T, T // 2):
            sq[b, first : first + T // 2, 0:H] = lax.dot_general(
                x[b, HALO + first : HALO + first + T // 2], wd[...], (((1,), (1,)), ((), ())),
                preferred_element_type=F32,
            )
    for g in range(1, G):
        v_copy(g).start()
    for c in small:
        c.wait()
    pad[0:1, 0:H] = step_o[...]
    pad[8:9, 0:H] = decay[...]
    pad[16:17, 0:H] = skip[...]

    pl.semaphore_wait(barrier, PEERS - 1 + HEADS_AXIS - 1)

    @pl.when(me < PEERS - 1)
    def _():
        halo_copy(me + 1).start()

    @pl.when(me == 0)
    def _():
        x[:, 0:HALO, :] = jnp.zeros((B, HALO, D), BF16)

    s_copy.wait()
    v_copy(0).wait()
    tri = lax.broadcasted_iota(jnp.int32, (L, L), 0) >= lax.broadcasted_iota(jnp.int32, (L, L), 1)
    tri16 = jnp.where(tri, 1.0, 0.0).astype(BF16)
    tri3 = jnp.concatenate([tri16, tri16, tri16], axis=1)

    def step_sizes(b):
        z = sq[b] + pad[0:1]
        step = jnp.maximum(z, 0.0) + jnp.log1p(jnp.exp(-jnp.abs(z)))
        decayed = step * (pad[8:9] * (-LOG2E))
        log_step = jnp.log(step) * LOG2E
        before = jnp.zeros((1, 128), F32)
        for k in range(K):
            part = decayed[k * L : (k + 1) * L]
            hi, mid, low = split3(part)
            stacked = jnp.concatenate([hi, mid, low], axis=0).astype(BF16)
            cum = dot(tri3, stacked)
            last = cum[L - 1 : L]
            source = cum - log_step[k * L : (k + 1) * L]
            cums[b, k] = cum
            closing[b, k] = jnp.exp2(last - source)
            a2g[b, k] = packed(jnp.exp2(cum))
            cs_t[b, k] = jnp.transpose(source)[0:32]
            pad[24 + b * K + k : 25 + b * K + k] = jnp.exp2(last)
            pad[32 + b * K + k : 33 + b * K + k] = jnp.exp2(before)
            before = before + last
        logsend[b : b + 1] = before
        sq[b] = jnp.zeros_like(sq[b])

    def main_dot(b, weights, into):
        for first in range(HALO, R, T // 2):
            raw = dot(x[b, first : first + T // 2], weights).astype(BF16).astype(F32)
            for j in range(2):
                into[b, j, first : first + T // 2] = raw[:, j * 128 : (j + 1) * 128]

    def halo_dot(weights, into):
        raw = dot(x[:, 0:HALO].reshape(B * HALO, D), weights).astype(BF16).astype(F32)
        for b in range(B):
            for j in range(2):
                into[b, j, 0:HALO] = raw[b * HALO : (b + 1) * HALO, j * 128 : (j + 1) * 128]

    for b in range(B):
        main_dot(b, ws[...], cm)
    for b in range(B):
        step_sizes(b)
        main_dot(b, wv[0], cv)

    def log_copy(dest):
        return pltpu.make_async_remote_copy(
            src_ref=logsend,
            dst_ref=logrecv.at[me],
            send_sem=lsem.at[0],
            recv_sem=lsem.at[1],
            device_id={"seq": dest},
            device_id_type=MESH,
        )

    @pl.when(me > 0)
    def _():
        halo_copy(me).wait_recv()

    for d in range(1, PEERS):
        log_copy(lax.rem(me + d, PEERS)).start()
    logrecv[me] = logsend[...]

    def share_copy(g, dest):
        return pltpu.make_async_remote_copy(
            src_ref=sendbuf.at[g, dest],
            dst_ref=recvbuf.at[g, me],
            send_sem=ssem.at[g],
            recv_sem=rsem.at[g],
            device_id={"seq": dest},
            device_id_type=MESH,
        )

    def back_copy(g, dest):
        return pltpu.make_async_remote_copy(
            src_ref=retbuf.at[g, dest],
            dst_ref=retrecv.at[g, me],
            send_sem=tsem.at[g],
            recv_sem=usem.at[g],
            device_id={"seq": dest},
            device_id_type=MESH,
        )

    first_half = lax.broadcasted_iota(jnp.int32, (L, 128), 1) < 64

    def to_front(heads, g):
        return pltpu.roll(heads, lax.rem(128 - 4 * g, 128), 1)

    def column(heads, n):
        return jnp.broadcast_to(heads[:, n : n + 1], (L, 128))

    def value_dot(g, b):
        for first in range(0, R, R // 2):
            raw = dot(x[b, first : first + R // 2], wv[g]).astype(BF16).astype(F32)
            for j in range(2):
                cv[b, j, first : first + R // 2] = raw[:, j * 128 : (j + 1) * 128]

    def value_conv(g, b):
        for j in range(2):
            at = pl.ds(pl.multiple_of(g * GC + j * 128, 128), 128)
            vbuf[g, b, :, j * 128 : (j + 1) * 128] = convolve(
                cv, b, value_k[:, at], value_o[pl.ds(2 * g + j, 1), :], j
            )

    def value_state(g, b):
        state = None
        for k in range(K):
            near = to_front(closing[b, k], g)
            scale = jnp.concatenate(
                [jnp.where(first_half, column(near, 2 * j), column(near, 2 * j + 1)) for j in range(2)],
                axis=1,
            )
            vk = vbuf[g, b, k * L : (k + 1) * L].astype(F32)
            made = dot(brow_t[b, k], (vk * scale).astype(BF16))
            if state is None:
                state = made
            else:
                local[g, b, k - 1] = state
                state = state * rows_t[g, b * K + k : b * K + k + 1] + made
        state = state.astype(BF16)
        for h in range(2):
            first = (b * 2 + h) * 8
            sendbuf[g, first : first + 8] = state[:, h * 128 : (h + 1) * 128].reshape(8, 16, 128)

    def send_shares(g):
        for d in range(1, PEERS):
            share_copy(g, lax.rem(me + d, PEERS)).start()
        recvbuf[g, me] = sendbuf[g, me]

    def convolve(raw, b, taps, offset, j):
        total = offset
        for tap in range(TAPS):
            total = total + taps[tap : tap + 1] * raw[b, j, pl.ds(HALO - TAPS + 1 + tap, T), :]
        return silu(total).astype(BF16)

    def bulk(buf, g, send, recv):
        return pltpu.make_async_remote_copy(
            src_ref=buf.at[g, pl.ds(0, PEERS - 1)],
            dst_ref=buf.at[g, pl.ds(0, PEERS - 1)],
            send_sem=send.at[g],
            recv_sem=recv.at[g],
            device_id={"seq": me},
            device_id_type=MESH,
        )

    def gate_dot(g, b):
        for first in range(0, T, T // 2):
            rows = slice(first, first + T // 2)
            gbuf[g, b, rows] = dot(x[b, HALO + first : HALO + first + T // 2], wg[g]).astype(BF16)

    def within(g, b):
        for k in range(K):
            rows = slice(k * L, (k + 1) * L)
            near = to_front(cums[b, k], g)
            for p in range(2):
                lanes = slice(p * 128, (p + 1) * 128)
                mixes = []
                for q in range(2):
                    n = 2 * p + q
                    spread = column(near, n) - cs_t[b, k, pl.ds(4 * g + n, 1), :]
                    mixes.append((jnp.exp2(jnp.minimum(spread, 100.0)) * sc[b, k]).astype(BF16))
                mix = jnp.concatenate(mixes, axis=1)
                v = vbuf[g, b, rows, lanes].astype(F32)
                two = jnp.concatenate(
                    [jnp.where(first_half, v, 0.0), jnp.where(first_half, 0.0, v)], axis=0
                ).astype(BF16)
                mixbuf[g, b, rows, lanes] = dot(mix, two) + rows_s[g, 0:1, lanes] * v

    def chain_share(g):
        chain = jnp.zeros((16, 128), F32)
        for j in range(PEERS):
            retbuf[g, j] = chain.astype(BF16)
            chain = chain * fac[g, j : j + 1] + recvbuf[g, j].astype(F32)

        for d in range(1, PEERS):
            back_copy(g, lax.rem(me + d, PEERS)).start()
        retrecv[g, me] = retbuf[g, me]

    def carry(g, b):
        halves = [
            retrecv[g, (b * 2 + h) * 8 : (b * 2 + h) * 8 + 8].reshape(128, 128) for h in range(2)
        ]
        entering = jnp.concatenate(halves, axis=1).astype(F32)
        for k in range(K):
            rows = slice(k * L, (k + 1) * L)
            if k == 0:
                state = entering
            else:
                state = local[g, b, k - 1] + entering * rows_b[g, b * K + k : b * K + k + 1]
            carried = dot(crow[b, k], state.astype(BF16))
            inside = dot(a2g[b, k], e256[g])
            mixture = mixbuf[g, b, rows] + inside * carried
            gated = mixture * silu(gbuf[g, b, rows].astype(F32))
            mixbuf[g, b, rows] = gated
            square = gated * gated
            sq[b, rows] = sq[b, rows] + square[:, 0:128] + square[:, 128:256]

    v_copy(1).wait()
    halo_dot(ws[...], cm)
    halo_dot(wv[0], cv)
    rt = packed(pad[24:32])
    rb = packed(pad[32:40])
    rs = packed(pad[16:24])
    for g in range(G):
        rows_t[g] = dot(rt, e256[g])
        rows_b[g] = dot(rb, e256[g])
        rows_s[g] = dot(rs, e256[g])
    for b in range(B):
        bmap = convolve(cm, b, state_k[:, 0:N], state_o[0:1], 0)
        cmap = convolve(cm, b, state_k[:, N : 2 * N], state_o[1:2], 1)
        for k in range(K):
            crow[b, k] = cmap[k * L : (k + 1) * L]
            brow_t[b, k] = jnp.transpose(bmap[k * L : (k + 1) * L].astype(F32)).astype(BF16)
        value_conv(0, b)
    for b in range(B):
        value_dot(1, b)
        for k in range(K):
            sc[b, k] = jnp.where(tri, dot(crow[b, k], brow_t[b, k]), 0.0)
        value_state(0, b)
    for g in range(G):
        g_copy(g).start()

    def value_group(g, _):
        v_copy(g).wait()
        send_shares(g - 2)
        for b in range(B):
            value_conv(g - 1, b)
        for b in range(B):
            value_dot(g, b)
            value_state(g - 1, b)
        return 0

    lax.fori_loop(2, G, value_group, 0)

    def all_logs():
        return pltpu.make_async_remote_copy(
            src_ref=logrecv.at[pl.ds(0, PEERS - 1)],
            dst_ref=logrecv.at[pl.ds(0, PEERS - 1)],
            send_sem=lsem.at[0],
            recv_sem=lsem.at[1],
            device_id={"seq": me},
            device_id_type=MESH,
        )

    def arrived(g):
        bulk(recvbuf, g, ssem, rsem).wait_recv()

    def returned(g):
        bulk(retrecv, g, tsem, usem).wait_recv()

    all_logs().wait_recv()
    my_batch = me // 16
    my_half = lax.rem(me // 8, 2)
    logs = logrecv[:, pl.ds(my_batch, 1), :].reshape(PEERS, 128)
    through = packed(jnp.exp2(logs))
    for g in range(G):
        fac[g] = dot(through, eh[my_half, g])

    g_copy(0).wait()
    arrived(0)
    send_shares(3)
    chain_share(0)
    for b in range(B):
        value_conv(4, b)
    for b in range(B):
        gate_dot(0, b)
        value_state(4, b)

    g_copy(1).wait()
    arrived(1)
    send_shares(4)
    chain_share(1)
    for b in range(B):
        gate_dot(1, b)
        within(b, 0)
        within(b, 1)

    g_copy(2).wait()
    arrived(2)
    arrived(3)
    chain_share(2)
    chain_share(3)
    for b in range(B):
        gate_dot(2, b)
        within(2 + b, 0)
        within(2 + b, 1)

    g_copy(3).wait()
    arrived(4)
    returned(0)
    chain_share(4)
    for b in range(B):
        carry(0, b)
        gate_dot(3, b)
        within(4, b)

    g_copy(4).wait()
    returned(1)
    returned(2)
    for b in range(B):
        carry(1 + b, 0)
        gate_dot(4, b)
        carry(1 + b, 1)

    returned(3)
    returned(4)
    for b in range(B):
        carry(3, b)
        carry(4, b)

    ones = jnp.ones((8, 256), BF16)
    for b in range(B):
        hi, mid, _ = split3(sq[b])
        terms = jnp.concatenate([hi, mid], axis=1).astype(BF16)
        ssend[b] = lax.dot_general(ones, terms, (((1,), (1,)), ((), ())), preferred_element_type=F32)

    def square_copy(d):
        return pltpu.make_async_remote_copy(
            src_ref=ssend,
            dst_ref=srecv.at[hd],
            send_sem=qsem.at[0],
            recv_sem=qsem.at[1],
            device_id={"head": lax.rem(hd + d, HEADS_AXIS)},
            device_id_type=MESH,
        )

    for d in range(1, HEADS_AXIS):
        square_copy(d).start()
    srecv[hd] = ssend[...]
    pltpu.make_async_remote_copy(
        src_ref=srecv.at[pl.ds(0, HEADS_AXIS - 1)],
        dst_ref=srecv.at[pl.ds(0, HEADS_AXIS - 1)],
        send_sem=qsem.at[0],
        recv_sem=qsem.at[1],
        device_id={"head": hd},
        device_id_type=MESH,
    ).wait_recv()
    eighth = jnp.full((16, 128), 0.125, BF16)
    for b in range(B):
        total = srecv[0, b] + srecv[1, b] + srecv[2, b] + srecv[3, b]
        inverse = lax.rsqrt(total / INNER + EPS)
        hi, mid, _ = split3(inverse)
        terms = jnp.concatenate([hi, mid], axis=0).astype(BF16)
        inverse_out[b] = lax.dot_general(terms, eighth, (((0,), (0,)), ((), ())), preferred_element_type=F32)

    def finish(g, _):
        bulk(sendbuf, g, ssem, rsem).wait_send()
        bulk(retbuf, g, tsem, usem).wait_send()
        return 0

    lax.fori_loop(0, G, finish, 0)
    all_logs().wait_send()
    pltpu.make_async_remote_copy(
        src_ref=srecv.at[pl.ds(0, HEADS_AXIS - 1)],
        dst_ref=srecv.at[pl.ds(0, HEADS_AXIS - 1)],
        send_sem=qsem.at[0],
        recv_sem=qsem.at[1],
        device_id={"head": hd},
        device_id_type=MESH,
    ).wait_send()

    @pl.when(me < PEERS - 1)
    def _():
        halo_copy(me + 1).wait_send()


def scale(gated, inverse, gain, out, obuf, sem):
    copies = []
    for g in range(G):
        for b in range(B):
            for j in range(2):
                lanes = slice(j * 128, (j + 1) * 128)
                obuf[g, b, :, lanes] = (
                    gated[g, b, :, lanes] * inverse[b] * gain[2 * g + j : 2 * g + j + 1]
                ).astype(BF16)
            copies.append(
                pltpu.make_async_copy(
                    obuf.at[g, b], out.at[b, :, pl.ds(g * GC, GC)], sem.at[g, b]
                )
            )
            copies[-1].start()
    for c in copies:
        c.wait()


def local_program(
    tokens, gate_weight, value_weight, state_weight, step_weight, value_kernel, value_offset,
    state_kernel, state_offset, step_offset, decay_rate, skip_gain, norm_gain,
):
    anywhere = pl.BlockSpec(memory_space=pl.ANY)
    inside = pl.BlockSpec(memory_space=pltpu.VMEM)
    vm = pltpu.VMEM
    dma = pltpu.SemaphoreType.DMA
    gated, inverse = pl.pallas_call(
        body,
        out_shape=(vm((G, B, T, GC), F32), vm((B, T, 128), F32)),
        in_specs=[anywhere] * 12,
        out_specs=(inside, inside),
        scratch_shapes=[
            vm((TAPS, C), F32),
            vm((C // 128, 128), F32),
            vm((TAPS, 2 * N), F32),
            vm((2, N), F32),
            vm((1, H), F32),
            vm((1, H), F32),
            vm((1, H), F32),
            vm((B, R, D), BF16),
            vm((G, D, GC), BF16),
            vm((G, D, GC), BF16),
            vm((D, 2 * N), BF16),
            vm((H, D), BF16),
            vm((B, 2, R, 128), F32),
            vm((B, 2, R, 128), F32),
            vm((G, B, T, GC), BF16),
            vm((G, B, T, GC), BF16),
            vm((B, K, N, L), BF16),
            vm((B, K, L, N), BF16),
            vm((B, K, L, L), F32),
            vm((B, K, L, 128), F32),
            vm((B, K, L, 128), F32),
            vm((B, K, L, 128), BF16),
            vm((B, K, 32, L), F32),
            vm((G, 128, 256), BF16),
            vm((2, G, 128, 128), BF16),
            vm((G, 8, GC), F32),
            vm((G, 8, GC), F32),
            vm((G, 8, GC), F32),
            vm((40, 128), F32),
            vm((G, B, K - 1, N, GC), F32),
            vm((G, PEERS, 16, 128), BF16),
            vm((G, PEERS, 16, 128), BF16),
            vm((G, PEERS, 16, 128), BF16),
            vm((G, PEERS, 16, 128), BF16),
            vm((8, 128), F32),
            vm((PEERS, 8, 128), F32),
            vm((G, PEERS, 128), F32),
            vm((B, T, 128), F32),
            vm((B, 8, T), F32),
            vm((HEADS_AXIS, B, 8, T), F32),
            dma((B,)), dma((G,)), dma((G,)), dma((2,)), dma((7,)), dma((2,)),
            dma((G,)), dma((G,)), dma((G,)), dma((G,)), dma((2,)), dma((2,)),
        ],
        compiler_params=pltpu.CompilerParams(
            collective_id=0, has_side_effects=True, vmem_limit_bytes=50 * 1024 * 1024
        ),
        name="mixer",
    )(
        tokens, gate_weight, value_weight, state_weight, step_weight.T, value_kernel,
        value_offset.reshape(C // 128, 128), state_kernel, state_offset.reshape(2, N),
        step_offset.reshape(1, H), decay_rate.reshape(1, H), skip_gain.reshape(1, H),
    )
    return pl.pallas_call(
        scale,
        out_shape=jax.ShapeDtypeStruct((B, T, C), BF16),
        in_specs=[inside] * 3,
        out_specs=anywhere,
        scratch_shapes=[vm((G, B, T, GC), BF16), dma((G, B))],
        compiler_params=pltpu.CompilerParams(vmem_limit_bytes=8 * 1024 * 1024),
        name="scale",
    )(gated, inverse, norm_gain.reshape(C // 128, 128))


def solution(mesh):
    return jax.shard_map(
        local_program,
        mesh=mesh,
        in_specs=(
            P(None, "seq", None),
            P(None, "head"),
            P(None, "head"),
            P(),
            P(None, "head"),
            P(None, "head"),
            P("head"),
            P(),
            P(),
            P("head"),
            P("head"),
            P("head"),
            P("head"),
        ),
        out_specs=P(None, "seq", "head"),
        check_vma=False,
    )
```

```python
import functools

import jax
import jax.numpy as jnp
from jax import lax
from jax.experimental import pallas as pl
from jax.experimental.pallas import tpu as pltpu
from jax.sharding import PartitionSpec as P

MESH = pl.DeviceIdType.MESH
F32 = jnp.float32
BF16 = jnp.bfloat16

EPS = 1e-05
LOG2E = 1.4426950408889634
B = 2
T = 512
D = 2560
C = 1280
H = 20
N = 128
L = 128
K = T // L
GC = 256
G = C // GC
HALO = 16
R = T + HALO
TAPS = 4
LUMPS = ((0, 2), (2, 1), (3, 1), (4, 1), (5, 1))
PEERS = 32
CHIPS = 16
HEADS_AXIS = 4
INNER = 5120


def dot(a, b):
    return jnp.dot(a, b, preferred_element_type=F32)


def split3(x):
    hi = x.astype(BF16).astype(F32)
    rest = x - hi
    mid = rest.astype(BF16).astype(F32)
    return hi, mid, rest - mid


def packed(x):
    lane = lax.broadcasted_iota(jnp.int32, x.shape, 1)
    hi, mid, low = split3(jnp.where(lane < H, x, 0.0))
    return (hi + pltpu.roll(mid, 32, 1) + pltpu.roll(low, 64, 1)).astype(BF16)


def silu(x):
    half = 0.5 * x
    return half * jnp.tanh(half) + half


def spread_matrix(shape, first_head, width):
    row = lax.broadcasted_iota(jnp.int32, shape, 0)
    col = lax.broadcasted_iota(jnp.int32, shape, 1)
    hit = (row & 31) == (first_head + col // width)
    return jnp.where(hit & (row < 96), 1.0, 0.0).astype(BF16)


def body(
    tok, gate_w, value_w, state_w, step_w,
    value_k_in, value_o_in, state_k_in, state_o_in, step_o_in, decay_in, skip_in,
    mixbuf, inverse_out,
    value_k, value_o, state_k, state_o, step_o, decay, skip,
    x, wv, wg, ws, wd, cv, cm, vbuf, gbuf, brow_t, crow, sc, cums, closing, a2g, cs_t,
    e256, eh, rows_t, rows_b, rows_s, pad, local, pairsend, pairrecv, logs_out, logs_in, rows_c, sendbuf, recvbuf, retbuf, retrecv,
    fac, sq, ssend, srecv,
    xsem, vsem, gsem, msem, psem, hsem,
    wsem, zsem, lsem, ssem, rsem, tsem, usem, qsem,
):
    me = lax.axis_index("seq")
    hd = lax.axis_index("head")
    core = lax.rem(me, 2)
    chip = lax.div(me, 2)
    partner = me + 1 - 2 * core

    x_copies = [
        pltpu.make_async_copy(tok.at[b], x.at[b, pl.ds(HALO, T)], xsem.at[b]) for b in range(B)
    ]
    s_copy = pltpu.make_async_copy(state_w, ws, msem.at[0])
    d_copy = pltpu.make_async_copy(step_w, wd, msem.at[1])

    def v_copy(g):
        return pltpu.make_async_copy(
            value_w.at[:, pl.ds(pl.multiple_of(g * GC, GC), GC)], wv.at[g], vsem.at[g]
        )

    def g_copy(g):
        return pltpu.make_async_copy(
            gate_w.at[:, pl.ds(pl.multiple_of(g * GC, GC), GC)], wg.at[g], gsem.at[g]
        )

    small = [
        pltpu.make_async_copy(src, dst, psem.at[i])
        for i, (src, dst) in enumerate(
            (
                (step_o_in, step_o), (decay_in, decay), (skip_in, skip), (state_k_in, state_k),
                (state_o_in, state_o), (value_k_in, value_k), (value_o_in, value_o),
            )
        )
    ]
    d_copy.start()
    for c in x_copies:
        c.start()
    for c in small:
        c.start()
    s_copy.start()
    v_copy(0).start()

    barrier = pltpu.get_barrier_semaphore()

    def greet(d, _):
        pl.semaphore_signal(
            barrier, inc=1, device_id={"seq": lax.rem(me + d, PEERS)}, device_id_type=MESH
        )
        return 0

    lax.fori_loop(1, PEERS, greet, 0)
    for d in range(1, HEADS_AXIS):
        pl.semaphore_signal(
            barrier, inc=1, device_id={"head": lax.rem(hd + d, HEADS_AXIS)}, device_id_type=MESH
        )

    for g in range(G):
        e256[g] = spread_matrix((128, 256), 4 * g, 64)
        for h in range(2):
            eh[h, g] = spread_matrix((128, 128), 2 * (2 * g + h), 64)
    pad[...] = jnp.zeros_like(pad)
    sq[...] = jnp.zeros_like(sq)
    retbuf[:, 0] = jnp.zeros((CHIPS, 16, 128), BF16)
    logs_out[...] = jnp.zeros_like(logs_out)

    def halo_copy(dest):
        return pltpu.make_async_remote_copy(
            src_ref=tok.at[:, pl.ds(T - HALO, HALO)],
            dst_ref=x.at[:, pl.ds(0, HALO)],
            send_sem=hsem.at[0],
            recv_sem=hsem.at[1],
            device_id={"seq": dest},
            device_id_type=MESH,
        )

    d_copy.wait()
    for b in range(B):
        x_copies[b].wait()
        for first in range(0, T, T // 2):
            sq[b, first : first + T // 2, 0:H] = lax.dot_general(
                x[b, HALO + first : HALO + first + T // 2], wd[...], (((1,), (1,)), ((), ())),
                preferred_element_type=F32,
            )
    for g in range(1, G):
        v_copy(g).start()
    for c in small:
        c.wait()
    pad[0:1, 0:H] = step_o[...]
    pad[8:9, 0:H] = decay[...]
    pad[16:17, 0:H] = skip[...]

    pl.semaphore_wait(barrier, PEERS - 1 + HEADS_AXIS - 1)

    @pl.when(me < PEERS - 1)
    def _():
        halo_copy(me + 1).start()

    @pl.when(me == 0)
    def _():
        x[:, 0:HALO, :] = jnp.zeros((B, HALO, D), BF16)

    s_copy.wait()
    v_copy(0).wait()
    tri = lax.broadcasted_iota(jnp.int32, (L, L), 0) >= lax.broadcasted_iota(jnp.int32, (L, L), 1)
    tri16 = jnp.where(tri, 1.0, 0.0).astype(BF16)
    tri3 = jnp.concatenate([tri16, tri16, tri16], axis=1)

    def step_sizes(b):
        z = sq[b] + pad[0:1]
        step = jnp.maximum(z, 0.0) + jnp.log1p(jnp.exp(-jnp.abs(z)))
        decayed = step * (pad[8:9] * (-LOG2E))
        log_step = jnp.log(step) * LOG2E
        before = jnp.zeros((1, 128), F32)
        for k in range(K):
            part = decayed[k * L : (k + 1) * L]
            hi, mid, low = split3(part)
            stacked = jnp.concatenate([hi, mid, low], axis=0).astype(BF16)
            cum = dot(tri3, stacked)
            last = cum[L - 1 : L]
            source = cum - log_step[k * L : (k + 1) * L]
            cums[b, k] = cum
            closing[b, k] = jnp.exp2(last - source)
            a2g[b, k] = packed(jnp.exp2(cum))
            cs_t[b, k] = jnp.transpose(source)[0:32]
            pad[24 + b * K + k : 25 + b * K + k] = jnp.exp2(last)
            pad[32 + b * K + k : 33 + b * K + k] = jnp.exp2(before)
            before = before + last
        logs_out[b : b + 1] = before
        sq[b] = jnp.zeros_like(sq[b])

    def main_dot(b, weights, into):
        for first in range(HALO, R, T // 2):
            raw = dot(x[b, first : first + T // 2], weights).astype(BF16).astype(F32)
            for j in range(2):
                into[b, j, first : first + T // 2] = raw[:, j * 128 : (j + 1) * 128]

    def halo_dot(weights, into):
        raw = dot(x[:, 0:HALO].reshape(B * HALO, D), weights).astype(BF16).astype(F32)
        for b in range(B):
            for j in range(2):
                into[b, j, 0:HALO] = raw[b * HALO : (b + 1) * HALO, j * 128 : (j + 1) * 128]

    for b in range(B):
        main_dot(b, ws[...], cm)
    for b in range(B):
        step_sizes(b)
        main_dot(b, wv[0], cv)

    def log_copy():
        return pltpu.make_async_remote_copy(
            src_ref=logs_out,
            dst_ref=logs_in,
            send_sem=lsem.at[0],
            recv_sem=lsem.at[1],
            device_id={"seq": partner},
            device_id_type=MESH,
        )

    log_copy().start()

    @pl.when(me > 0)
    def _():
        halo_copy(me).wait_recv()

    def tiles(buf, lump, at):
        first, count = LUMPS[lump]
        return buf.at[at, pl.ds(first, count)]

    def pair_copy(g):
        return pltpu.make_async_remote_copy(
            src_ref=pairsend.at[g],
            dst_ref=pairrecv.at[g],
            send_sem=wsem.at[g],
            recv_sem=zsem.at[g],
            device_id={"seq": partner},
            device_id_type=MESH,
        )

    def share_copy(lump, to_chip):
        return pltpu.make_async_remote_copy(
            src_ref=tiles(sendbuf, lump, to_chip),
            dst_ref=tiles(recvbuf, lump, chip),
            send_sem=ssem.at[lump],
            recv_sem=rsem.at[lump],
            device_id={"seq": 2 * to_chip + core},
            device_id_type=MESH,
        )

    def back_copy(lump, dest):
        return pltpu.make_async_remote_copy(
            src_ref=tiles(retbuf, lump, lax.div(dest, 2)),
            dst_ref=tiles(retrecv, lump, core * CHIPS + chip),
            send_sem=tsem.at[lump],
            recv_sem=usem.at[lump],
            device_id={"seq": dest},
            device_id_type=MESH,
        )

    first_half = lax.broadcasted_iota(jnp.int32, (L, 128), 1) < 64

    def to_front(heads, g):
        return pltpu.roll(heads, lax.rem(128 - 4 * g, 128), 1)

    def column(heads, n):
        return jnp.broadcast_to(heads[:, n : n + 1], (L, 128))

    def value_dot(g, b):
        for first in range(0, R, R // 2):
            raw = dot(x[b, first : first + R // 2], wv[g]).astype(BF16).astype(F32)
            for j in range(2):
                cv[b, j, first : first + R // 2] = raw[:, j * 128 : (j + 1) * 128]

    def value_conv(g, b):
        for j in range(2):
            at = pl.ds(pl.multiple_of(g * GC + j * 128, 128), 128)
            vbuf[g, b, :, j * 128 : (j + 1) * 128] = convolve(
                cv, b, value_k[:, at], value_o[pl.ds(2 * g + j, 1), :], j
            )

    def value_state(g, b):
        state = None
        for k in range(K):
            near = to_front(closing[b, k], g)
            scale = jnp.concatenate(
                [jnp.where(first_half, column(near, 2 * j), column(near, 2 * j + 1)) for j in range(2)],
                axis=1,
            )
            vk = vbuf[g, b, k * L : (k + 1) * L].astype(F32)
            made = dot(brow_t[b, k], (vk * scale).astype(BF16))
            if state is None:
                state = made
            else:
                local[g, b, k - 1] = state
                state = state * rows_t[g, b * K + k : b * K + k + 1] + made
        pairsend[g, b] = state.astype(BF16)

    def chip_decays():
        log_copy().wait_recv()
        second_core = core == 1
        early = jnp.where(second_core, logs_in[...], logs_out[...])
        late = jnp.where(second_core, logs_out[...], logs_in[...])
        both = jnp.exp2(early + late)
        both = jnp.where(second_core, both[1:2], both[0:1])
        sendbuf[:, 0] = jnp.broadcast_to(
            packed(jnp.broadcast_to(both, (16, 128)))[None], (CHIPS, 16, 128)
        )
        late = jnp.where(second_core, late[1:2], late[0:1])
        none = jnp.zeros((1, 128), F32)
        pad[40:41] = jnp.where(second_core, none, late)
        pad[41:42] = jnp.where(second_core, late, none)
        pad[42:44] = jnp.where(second_core, early[0:2], jnp.zeros((2, 128), F32))
        factors = packed(jnp.exp2(pad[40:48]))
        for g in range(G):
            rows_c[g] = dot(factors, e256[g])

    def send_shares(lump):
        pair_copy(lump).wait_recv()
        whole = (
            rows_c[lump, 0:1] * pairsend[lump, core].astype(F32)
            + rows_c[lump, 1:2] * pairrecv[lump, core].astype(F32)
        ).astype(BF16)
        for h in range(2):
            sendbuf[h * 8 : h * 8 + 8, lump + 1] = whole[:, h * 128 : (h + 1) * 128].reshape(8, 16, 128)
        for d in range(1, CHIPS):
            ahead = chip + d
            share_copy(lump, jnp.where(ahead < CHIPS, ahead, ahead - CHIPS)).start()
        first, count = LUMPS[lump]
        recvbuf[chip, first : first + count] = sendbuf[chip, first : first + count]

    def convolve(raw, b, taps, offset, j):
        total = offset
        for tap in range(TAPS):
            total = total + taps[tap : tap + 1] * raw[b, j, pl.ds(HALO - TAPS + 1 + tap, T), :]
        return silu(total).astype(BF16)

    def bulk(buf, lump, count, send, recv):
        return pltpu.make_async_remote_copy(
            src_ref=tiles(buf, lump, pl.ds(0, count)),
            dst_ref=tiles(buf, lump, pl.ds(0, count)),
            send_sem=send.at[lump],
            recv_sem=recv.at[lump],
            device_id={"seq": me},
            device_id_type=MESH,
        )

    def gate_dot(g, b):
        for first in range(0, T, T // 2):
            rows = slice(first, first + T // 2)
            gbuf[g, b, rows] = dot(x[b, HALO + first : HALO + first + T // 2], wg[g]).astype(BF16)

    def within(g, b):
        for k in range(K):
            rows = slice(k * L, (k + 1) * L)
            near = to_front(cums[b, k], g)
            for p in range(2):
                lanes = slice(p * 128, (p + 1) * 128)
                mixes = []
                for q in range(2):
                    n = 2 * p + q
                    spread = column(near, n) - cs_t[b, k, pl.ds(4 * g + n, 1), :]
                    mixes.append(jnp.exp2(jnp.minimum(spread, 100.0)).astype(BF16) * sc[b, k])
                mix = jnp.concatenate(mixes, axis=1)
                v = vbuf[g, b, rows, lanes].astype(F32)
                two = jnp.concatenate(
                    [jnp.where(first_half, v, 0.0), jnp.where(first_half, 0.0, v)], axis=0
                ).astype(BF16)
                mixbuf[g, b, rows, lanes] = dot(mix, two) + rows_s[g, 0:1, lanes] * v

    def chain_share(lump):
        first, count = LUMPS[lump]
        chain = jnp.zeros((16, 128), F32)
        for j in range(CHIPS):
            retbuf[j, lump + 1] = chain.astype(BF16)
            chain = chain * fac[lump, j] + recvbuf[j, lump + 1].astype(F32)
        for d in range(1, PEERS):
            ahead = me + d
            back_copy(lump, jnp.where(ahead < PEERS, ahead, ahead - PEERS)).start()
        retrecv[core * CHIPS + chip, first : first + count] = retbuf[chip, first : first + count]

    def carry(g, b):
        halves = [
            retrecv[(b * 2 + h) * 8 : (b * 2 + h) * 8 + 8, g + 1].reshape(128, 128) for h in range(2)
        ]
        entering = rows_c[g, 2 + b : 3 + b] * jnp.concatenate(halves, axis=1).astype(F32)
        entering = entering + core.astype(F32) * pairrecv[g, b].astype(F32)
        for k in range(K):
            rows = slice(k * L, (k + 1) * L)
            if k == 0:
                state = entering
            else:
                state = local[g, b, k - 1] + entering * rows_b[g, b * K + k : b * K + k + 1]
            carried = dot(crow[b, k], state.astype(BF16))
            inside = dot(a2g[b, k], e256[g])
            mixture = mixbuf[g, b, rows] + inside * carried
            gated = mixture * silu(gbuf[g, b, rows].astype(F32))
            mixbuf[g, b, rows] = gated
            square = gated * gated
            sq[b, rows] = sq[b, rows] + square[:, 0:128] + square[:, 128:256]

    v_copy(1).wait()
    halo_dot(ws[...], cm)
    halo_dot(wv[0], cv)
    rt = packed(pad[24:32])
    rb = packed(pad[32:40])
    rs = packed(pad[16:24])
    for g in range(G):
        rows_t[g] = dot(rt, e256[g])
        rows_b[g] = dot(rb, e256[g])
        rows_s[g] = dot(rs, e256[g])
    for b in range(B):
        bmap = convolve(cm, b, state_k[:, 0:N], state_o[0:1], 0)
        cmap = convolve(cm, b, state_k[:, N : 2 * N], state_o[1:2], 1)
        for k in range(K):
            crow[b, k] = cmap[k * L : (k + 1) * L]
            brow_t[b, k] = jnp.transpose(bmap[k * L : (k + 1) * L].astype(F32)).astype(BF16)
        value_conv(0, b)
    for b in range(B):
        value_dot(1, b)
        for k in range(K):
            sc[b, k] = jnp.where(tri, dot(crow[b, k], brow_t[b, k]), 0.0).astype(BF16)
        value_state(0, b)
    for g in range(G):
        g_copy(g).start()

    for g in range(2, G):
        v_copy(g).wait()
        pair_copy(g - 2).start()
        if g == 3:
            chip_decays()
        if g > 2:
            send_shares(g - 3)
        for b in range(B):
            value_conv(g - 1, b)
        for b in range(B):
            value_dot(g, b)
            value_state(g - 1, b)

    def arrived(lump):
        bulk(recvbuf, lump, CHIPS - 1, ssem, rsem).wait_recv()

    def returned(lump):
        bulk(retrecv, lump, PEERS - 1, tsem, usem).wait_recv()

    g_copy(0).wait()
    pair_copy(3).start()
    send_shares(2)
    for b in range(B):
        value_conv(4, b)
    for b in range(B):
        gate_dot(0, b)
        value_state(4, b)

    g_copy(1).wait()
    pair_copy(4).start()
    send_shares(3)
    arrived(0)
    my_half = lax.div(chip, 8)
    through = recvbuf[:, 0].reshape(CHIPS * 16, 128)
    for g in range(G):
        fac[g] = dot(through, eh[my_half, g]).reshape(CHIPS, 16, 128)
    chain_share(0)
    for b in range(B):
        gate_dot(1, b)
        within(0, b)

    send_shares(4)
    arrived(1)
    arrived(2)
    chain_share(1)
    chain_share(2)
    g_copy(2).wait()
    for b in range(B):
        gate_dot(2, b)
        within(1, b)

    g_copy(3).wait()
    arrived(3)
    chain_share(3)
    for b in range(B):
        gate_dot(3, b)
        within(2, b)

    g_copy(4).wait()
    arrived(4)
    chain_share(4)
    for b in range(B):
        gate_dot(4, b)
        within(3, b)
        within(4, b)

    returned(0)
    returned(1)
    returned(2)
    for b in range(B):
        carry(0, b)
        carry(1, b)
        carry(2, b)

    returned(3)
    returned(4)
    for b in range(B):
        carry(3, b)
        carry(4, b)

    ones = jnp.ones((8, 256), BF16)
    for b in range(B):
        hi, mid, _ = split3(sq[b])
        terms = jnp.concatenate([hi, mid], axis=1).astype(BF16)
        ssend[b] = lax.dot_general(ones, terms, (((1,), (1,)), ((), ())), preferred_element_type=F32)

    def square_copy(d):
        return pltpu.make_async_remote_copy(
            src_ref=ssend,
            dst_ref=srecv.at[hd],
            send_sem=qsem.at[0],
            recv_sem=qsem.at[1],
            device_id={"head": lax.rem(hd + d, HEADS_AXIS)},
            device_id_type=MESH,
        )

    for d in range(1, HEADS_AXIS):
        square_copy(d).start()
    srecv[hd] = ssend[...]
    pltpu.make_async_remote_copy(
        src_ref=srecv.at[pl.ds(0, HEADS_AXIS - 1)],
        dst_ref=srecv.at[pl.ds(0, HEADS_AXIS - 1)],
        send_sem=qsem.at[0],
        recv_sem=qsem.at[1],
        device_id={"head": hd},
        device_id_type=MESH,
    ).wait_recv()
    eighth = jnp.full((16, 128), 0.125, BF16)
    for b in range(B):
        total = srecv[0, b] + srecv[1, b] + srecv[2, b] + srecv[3, b]
        inverse = lax.rsqrt(total / INNER + EPS)
        hi, mid, _ = split3(inverse)
        terms = jnp.concatenate([hi, mid], axis=0).astype(BF16)
        inverse_out[b] = lax.dot_general(terms, eighth, (((0,), (0,)), ((), ())), preferred_element_type=F32)

    log_copy().wait_send()
    for lump in range(G):
        pair_copy(lump).wait_send()
        bulk(sendbuf, lump, CHIPS - 1, ssem, rsem).wait_send()
        bulk(retrecv, lump, PEERS - 1, tsem, usem).wait_send()
    pltpu.make_async_remote_copy(
        src_ref=srecv.at[pl.ds(0, HEADS_AXIS - 1)],
        dst_ref=srecv.at[pl.ds(0, HEADS_AXIS - 1)],
        send_sem=qsem.at[0],
        recv_sem=qsem.at[1],
        device_id={"head": hd},
        device_id_type=MESH,
    ).wait_send()

    @pl.when(me < PEERS - 1)
    def _():
        halo_copy(me + 1).wait_send()


def scale(gated, inverse, gain, out, obuf, sem):
    copies = []
    for b in range(B):
        for k in range(K):
            rows = slice(k * L, (k + 1) * L)
            factor = inverse[b, rows]
            for g in range(G):
                for j in range(2):
                    first = g * GC + j * 128
                    obuf[b, rows, first : first + 128] = (
                        gated[g, b, rows, j * 128 : (j + 1) * 128]
                        * factor
                        * gain[2 * g + j : 2 * g + j + 1]
                    ).astype(BF16)
            copies.append(
                pltpu.make_async_copy(
                    obuf.at[b, pl.ds(k * L, L)], out.at[b, pl.ds(k * L, L)], sem.at[b, k]
                )
            )
            copies[-1].start()
    for c in copies:
        c.wait()


def local_program(
    tokens, gate_weight, value_weight, state_weight, step_weight, value_kernel, value_offset,
    state_kernel, state_offset, step_offset, decay_rate, skip_gain, norm_gain,
):
    anywhere = pl.BlockSpec(memory_space=pl.ANY)
    inside = pl.BlockSpec(memory_space=pltpu.VMEM)
    vm = pltpu.VMEM
    dma = pltpu.SemaphoreType.DMA
    gated, inverse = pl.pallas_call(
        body,
        out_shape=(vm((G, B, T, GC), F32), vm((B, T, 128), F32)),
        in_specs=[anywhere] * 12,
        out_specs=(inside, inside),
        scratch_shapes=[
            vm((TAPS, C), F32),
            vm((C // 128, 128), F32),
            vm((TAPS, 2 * N), F32),
            vm((2, N), F32),
            vm((1, H), F32),
            vm((1, H), F32),
            vm((1, H), F32),
            vm((B, R, D), BF16),
            vm((G, D, GC), BF16),
            vm((G, D, GC), BF16),
            vm((D, 2 * N), BF16),
            vm((H, D), BF16),
            vm((B, 2, R, 128), F32),
            vm((B, 2, R, 128), F32),
            vm((G, B, T, GC), BF16),
            vm((G, B, T, GC), BF16),
            vm((B, K, N, L), BF16),
            vm((B, K, L, N), BF16),
            vm((B, K, L, L), BF16),
            vm((B, K, L, 128), F32),
            vm((B, K, L, 128), F32),
            vm((B, K, L, 128), BF16),
            vm((B, K, 32, L), F32),
            vm((G, 128, 256), BF16),
            vm((2, G, 128, 128), BF16),
            vm((G, 8, GC), F32),
            vm((G, 8, GC), F32),
            vm((G, 8, GC), F32),
            vm((48, 128), F32),
            vm((G, B, K - 1, N, GC), F32),
            vm((G, B, N, GC), BF16),
            vm((G, B, N, GC), BF16),
            vm((8, 128), F32),
            vm((8, 128), F32),
            vm((G, 8, GC), F32),
            vm((CHIPS, G + 1, 16, 128), BF16),
            vm((CHIPS, G + 1, 16, 128), BF16),
            vm((CHIPS, G + 1, 16, 128), BF16),
            vm((PEERS, G + 1, 16, 128), BF16),
            vm((G, CHIPS, 16, 128), F32),
            vm((B, T, 128), F32),
            vm((B, 8, T), F32),
            vm((HEADS_AXIS, B, 8, T), F32),
            dma((B,)), dma((G,)), dma((G,)), dma((2,)), dma((7,)), dma((2,)),
            dma((G,)), dma((G,)), dma((2,)),
            dma((G,)), dma((G,)), dma((G,)), dma((G,)), dma((2,)),
        ],
        compiler_params=pltpu.CompilerParams(
            collective_id=0, has_side_effects=True, vmem_limit_bytes=50 * 1024 * 1024
        ),
        name="mixer",
    )(
        tokens, gate_weight, value_weight, state_weight, step_weight.T, value_kernel,
        value_offset.reshape(C // 128, 128), state_kernel, state_offset.reshape(2, N),
        step_offset.reshape(1, H), decay_rate.reshape(1, H), skip_gain.reshape(1, H),
    )
    return pl.pallas_call(
        scale,
        out_shape=jax.ShapeDtypeStruct((B, T, C), BF16),
        in_specs=[inside] * 3,
        out_specs=anywhere,
        scratch_shapes=[vm((B, T, C), BF16), dma((B, K))],
        compiler_params=pltpu.CompilerParams(vmem_limit_bytes=8 * 1024 * 1024),
        name="scale",
    )(gated, inverse, norm_gain.reshape(C // 128, 128))


def solution(mesh):
    return jax.shard_map(
        local_program,
        mesh=mesh,
        in_specs=(
            P(None, "seq", None),
            P(None, "head"),
            P(None, "head"),
            P(),
            P(None, "head"),
            P(None, "head"),
            P("head"),
            P(),
            P(),
            P("head"),
            P("head"),
            P("head"),
            P("head"),
        ),
        out_specs=P(None, "seq", "head"),
        check_vma=False,
    )
```

```python
import functools

import jax
import jax.numpy as jnp
from jax import lax
from jax.experimental import pallas as pl
from jax.experimental.pallas import tpu as pltpu
from jax.sharding import PartitionSpec as P

MESH = pl.DeviceIdType.MESH
F32 = jnp.float32
BF16 = jnp.bfloat16

EPS = 1e-05
LOG2E = 1.4426950408889634
B = 2
T = 512
D = 2560
C = 1280
H = 20
N = 128
L = 128
K = T // L
GC = 256
G = C // GC
HALO = 16
R = T + HALO
TAPS = 4
LUMPS = ((0, 2), (2, 1), (3, 1), (4, 1), (5, 1))
PEERS = 32
HEADS_AXIS = 4
INNER = 5120


def dot(a, b):
    return jnp.dot(a, b, preferred_element_type=F32)


def split3(x):
    hi = x.astype(BF16).astype(F32)
    rest = x - hi
    mid = rest.astype(BF16).astype(F32)
    return hi, mid, rest - mid


def packed(x):
    lane = lax.broadcasted_iota(jnp.int32, x.shape, 1)
    hi, mid, low = split3(jnp.where(lane < H, x, 0.0))
    return (hi + pltpu.roll(mid, 32, 1) + pltpu.roll(low, 64, 1)).astype(BF16)


def silu(x):
    half = 0.5 * x
    return half * jnp.tanh(half) + half


def spread_matrix(shape, first_head, width):
    row = lax.broadcasted_iota(jnp.int32, shape, 0)
    col = lax.broadcasted_iota(jnp.int32, shape, 1)
    hit = (row & 31) == (first_head + col // width)
    return jnp.where(hit & (row < 96), 1.0, 0.0).astype(BF16)


def body(
    tok, gate_w, value_w, state_w, step_w,
    value_k_in, value_o_in, state_k_in, state_o_in, step_o_in, decay_in, skip_in,
    mixbuf, inverse_out,
    value_k, value_o, state_k, state_o, step_o, decay, skip,
    x, wv, wg, ws, wd, cv, cm, vbuf, gbuf, brow_t, crow, sc, cums, closing, a2g, cs_t,
    e256, eh, rows_t, rows_b, rows_s, pad, local, sendbuf, recvbuf, retbuf, retrecv,
    fac, sq, ssend, srecv,
    xsem, vsem, gsem, msem, psem, hsem, ssem, rsem, tsem, usem, qsem,
):
    me = lax.axis_index("seq")
    hd = lax.axis_index("head")

    x_copies = [
        pltpu.make_async_copy(tok.at[b], x.at[b, pl.ds(HALO, T)], xsem.at[b]) for b in range(B)
    ]
    s_copy = pltpu.make_async_copy(state_w, ws, msem.at[0])
    d_copy = pltpu.make_async_copy(step_w, wd, msem.at[1])

    def v_copy(g):
        return pltpu.make_async_copy(
            value_w.at[:, pl.ds(pl.multiple_of(g * GC, GC), GC)], wv.at[g], vsem.at[g]
        )

    def g_copy(g):
        return pltpu.make_async_copy(
            gate_w.at[:, pl.ds(pl.multiple_of(g * GC, GC), GC)], wg.at[g], gsem.at[g]
        )

    small = [
        pltpu.make_async_copy(src, dst, psem.at[i])
        for i, (src, dst) in enumerate(
            (
                (step_o_in, step_o), (decay_in, decay), (skip_in, skip), (state_k_in, state_k),
                (state_o_in, state_o), (value_k_in, value_k), (value_o_in, value_o),
            )
        )
    ]
    d_copy.start()
    for c in x_copies:
        c.start()
    for c in small:
        c.start()
    s_copy.start()
    v_copy(0).start()

    barrier = pltpu.get_barrier_semaphore()

    def greet(d, _):
        pl.semaphore_signal(
            barrier, inc=1, device_id={"seq": lax.rem(me + d, PEERS)}, device_id_type=MESH
        )
        return 0

    lax.fori_loop(1, PEERS, greet, 0)
    for d in range(1, HEADS_AXIS):
        pl.semaphore_signal(
            barrier, inc=1, device_id={"head": lax.rem(hd + d, HEADS_AXIS)}, device_id_type=MESH
        )

    for g in range(G):
        e256[g] = spread_matrix((128, 256), 4 * g, 64)
        for h in range(2):
            eh[h, g] = spread_matrix((128, 128), 2 * (2 * g + h), 64)
    pad[...] = jnp.zeros_like(pad)
    sq[...] = jnp.zeros_like(sq)
    retbuf[:, 0] = jnp.zeros((PEERS, 16, 128), BF16)

    def halo_copy(dest):
        return pltpu.make_async_remote_copy(
            src_ref=tok.at[:, pl.ds(T - HALO, HALO)],
            dst_ref=x.at[:, pl.ds(0, HALO)],
            send_sem=hsem.at[0],
            recv_sem=hsem.at[1],
            device_id={"seq": dest},
            device_id_type=MESH,
        )

    d_copy.wait()
    for b in range(B):
        x_copies[b].wait()
        for first in range(0, T, T // 2):
            sq[b, first : first + T // 2, 0:H] = lax.dot_general(
                x[b, HALO + first : HALO + first + T // 2], wd[...], (((1,), (1,)), ((), ())),
                preferred_element_type=F32,
            )
    for g in range(1, G):
        v_copy(g).start()
    for c in small:
        c.wait()
    pad[0:1, 0:H] = step_o[...]
    pad[8:9, 0:H] = decay[...]
    pad[16:17, 0:H] = skip[...]

    pl.semaphore_wait(barrier, PEERS - 1 + HEADS_AXIS - 1)

    @pl.when(me < PEERS - 1)
    def _():
        halo_copy(me + 1).start()

    @pl.when(me == 0)
    def _():
        x[:, 0:HALO, :] = jnp.zeros((B, HALO, D), BF16)

    s_copy.wait()
    v_copy(0).wait()
    tri = lax.broadcasted_iota(jnp.int32, (L, L), 0) >= lax.broadcasted_iota(jnp.int32, (L, L), 1)
    tri16 = jnp.where(tri, 1.0, 0.0).astype(BF16)
    tri3 = jnp.concatenate([tri16, tri16, tri16], axis=1)

    def step_sizes(b):
        z = sq[b] + pad[0:1]
        step = jnp.maximum(z, 0.0) + jnp.log1p(jnp.exp(-jnp.abs(z)))
        decayed = step * (pad[8:9] * (-LOG2E))
        log_step = jnp.log(step) * LOG2E
        before = jnp.zeros((1, 128), F32)
        for k in range(K):
            part = decayed[k * L : (k + 1) * L]
            hi, mid, low = split3(part)
            stacked = jnp.concatenate([hi, mid, low], axis=0).astype(BF16)
            cum = dot(tri3, stacked)
            last = cum[L - 1 : L]
            source = cum - log_step[k * L : (k + 1) * L]
            cums[b, k] = cum
            closing[b, k] = jnp.exp2(last - source)
            a2g[b, k] = packed(jnp.exp2(cum))
            cs_t[b, k] = jnp.transpose(source)[0:32]
            pad[24 + b * K + k : 25 + b * K + k] = jnp.exp2(last)
            pad[32 + b * K + k : 33 + b * K + k] = jnp.exp2(before)
            before = before + last
        whole = packed(jnp.broadcast_to(jnp.exp2(before), (16, 128)))
        sendbuf[16 * b : 16 * b + 16, 0] = jnp.broadcast_to(whole[None], (16, 16, 128))
        sq[b] = jnp.zeros_like(sq[b])

    def main_dot(b, weights, into):
        for first in range(HALO, R, T // 2):
            raw = dot(x[b, first : first + T // 2], weights).astype(BF16).astype(F32)
            for j in range(2):
                into[b, j, first : first + T // 2] = raw[:, j * 128 : (j + 1) * 128]

    def halo_dot(weights, into):
        raw = dot(x[:, 0:HALO].reshape(B * HALO, D), weights).astype(BF16).astype(F32)
        for b in range(B):
            for j in range(2):
                into[b, j, 0:HALO] = raw[b * HALO : (b + 1) * HALO, j * 128 : (j + 1) * 128]

    for b in range(B):
        main_dot(b, ws[...], cm)
    for b in range(B):
        step_sizes(b)
        main_dot(b, wv[0], cv)

    @pl.when(me > 0)
    def _():
        halo_copy(me).wait_recv()

    def peer(d):
        ahead = me + d
        return jnp.where(ahead < PEERS, ahead, ahead - PEERS)

    def tiles(buf, lump, at):
        first, count = LUMPS[lump]
        return buf.at[at, pl.ds(first, count)]

    def share_copy(lump, dest):
        return pltpu.make_async_remote_copy(
            src_ref=tiles(sendbuf, lump, dest),
            dst_ref=tiles(recvbuf, lump, me),
            send_sem=ssem.at[lump],
            recv_sem=rsem.at[lump],
            device_id={"seq": dest},
            device_id_type=MESH,
        )

    def back_copy(lump, dest):
        return pltpu.make_async_remote_copy(
            src_ref=tiles(retbuf, lump, dest),
            dst_ref=tiles(retrecv, lump, me),
            send_sem=tsem.at[lump],
            recv_sem=usem.at[lump],
            device_id={"seq": dest},
            device_id_type=MESH,
        )

    first_half = lax.broadcasted_iota(jnp.int32, (L, 128), 1) < 64

    def to_front(heads, g):
        return pltpu.roll(heads, lax.rem(128 - 4 * g, 128), 1)

    def column(heads, n):
        return jnp.broadcast_to(heads[:, n : n + 1], (L, 128))

    def value_dot(g, b):
        for first in range(0, R, R // 2):
            raw = dot(x[b, first : first + R // 2], wv[g]).astype(BF16).astype(F32)
            for j in range(2):
                cv[b, j, first : first + R // 2] = raw[:, j * 128 : (j + 1) * 128]

    def value_conv(g, b):
        for j in range(2):
            at = pl.ds(pl.multiple_of(g * GC + j * 128, 128), 128)
            vbuf[g, b, :, j * 128 : (j + 1) * 128] = convolve(
                cv, b, value_k[:, at], value_o[pl.ds(2 * g + j, 1), :], j
            )

    def value_state(g, b):
        state = None
        for k in range(K):
            near = to_front(closing[b, k], g)
            scale = jnp.concatenate(
                [jnp.where(first_half, column(near, 2 * j), column(near, 2 * j + 1)) for j in range(2)],
                axis=1,
            )
            vk = vbuf[g, b, k * L : (k + 1) * L].astype(F32)
            made = dot(brow_t[b, k], (vk * scale).astype(BF16))
            if state is None:
                state = made
            else:
                local[g, b, k - 1] = state
                state = state * rows_t[g, b * K + k : b * K + k + 1] + made
        state = state.astype(BF16)
        for h in range(2):
            first = (b * 2 + h) * 8
            sendbuf[first : first + 8, g + 1] = state[:, h * 128 : (h + 1) * 128].reshape(8, 16, 128)

    def send_shares(lump):
        for d in range(1, PEERS):
            share_copy(lump, peer(d)).start()
        first, count = LUMPS[lump]
        recvbuf[me, first : first + count] = sendbuf[me, first : first + count]

    def convolve(raw, b, taps, offset, j):
        total = offset
        for tap in range(TAPS):
            total = total + taps[tap : tap + 1] * raw[b, j, pl.ds(HALO - TAPS + 1 + tap, T), :]
        return silu(total).astype(BF16)

    def bulk(buf, lump, send, recv):
        return pltpu.make_async_remote_copy(
            src_ref=tiles(buf, lump, pl.ds(0, PEERS - 1)),
            dst_ref=tiles(buf, lump, pl.ds(0, PEERS - 1)),
            send_sem=send.at[lump],
            recv_sem=recv.at[lump],
            device_id={"seq": me},
            device_id_type=MESH,
        )

    def gate_dot(g, b):
        for first in range(0, T, T // 2):
            rows = slice(first, first + T // 2)
            gbuf[g, b, rows] = dot(x[b, HALO + first : HALO + first + T // 2], wg[g]).astype(BF16)

    def within(g, b):
        for k in range(K):
            rows = slice(k * L, (k + 1) * L)
            near = to_front(cums[b, k], g)
            for p in range(2):
                lanes = slice(p * 128, (p + 1) * 128)
                mixes = []
                for q in range(2):
                    n = 2 * p + q
                    spread = column(near, n) - cs_t[b, k, pl.ds(4 * g + n, 1), :]
                    mixes.append(jnp.exp2(jnp.minimum(spread, 100.0)).astype(BF16) * sc[b, k])
                mix = jnp.concatenate(mixes, axis=1)
                v = vbuf[g, b, rows, lanes].astype(F32)
                two = jnp.concatenate(
                    [jnp.where(first_half, v, 0.0), jnp.where(first_half, 0.0, v)], axis=0
                ).astype(BF16)
                mixbuf[g, b, rows, lanes] = dot(mix, two) + rows_s[g, 0:1, lanes] * v

    def chain_share(lump):
        first, count = LUMPS[lump]
        for tile in range(max(first, 1), first + count):
            chain = jnp.zeros((16, 128), F32)
            for j in range(PEERS):
                retbuf[j, tile] = chain.astype(BF16)
                chain = chain * fac[tile - 1, j] + recvbuf[j, tile].astype(F32)

        for d in range(1, PEERS):
            back_copy(lump, peer(d)).start()
        retrecv[me, first : first + count] = retbuf[me, first : first + count]

    def carry(g, b):
        halves = [
            retrecv[(b * 2 + h) * 8 : (b * 2 + h) * 8 + 8, g + 1].reshape(128, 128) for h in range(2)
        ]
        entering = jnp.concatenate(halves, axis=1).astype(F32)
        for k in range(K):
            rows = slice(k * L, (k + 1) * L)
            if k == 0:
                state = entering
            else:
                state = local[g, b, k - 1] + entering * rows_b[g, b * K + k : b * K + k + 1]
            carried = dot(crow[b, k], state.astype(BF16))
            inside = dot(a2g[b, k], e256[g])
            mixture = mixbuf[g, b, rows] + inside * carried
            gated = mixture * silu(gbuf[g, b, rows].astype(F32))
            mixbuf[g, b, rows] = gated
            square = gated * gated
            sq[b, rows] = sq[b, rows] + square[:, 0:128] + square[:, 128:256]

    v_copy(1).wait()
    halo_dot(ws[...], cm)
    halo_dot(wv[0], cv)
    rt = packed(pad[24:32])
    rb = packed(pad[32:40])
    rs = packed(pad[16:24])
    for g in range(G):
        rows_t[g] = dot(rt, e256[g])
        rows_b[g] = dot(rb, e256[g])
        rows_s[g] = dot(rs, e256[g])
    for b in range(B):
        bmap = convolve(cm, b, state_k[:, 0:N], state_o[0:1], 0)
        cmap = convolve(cm, b, state_k[:, N : 2 * N], state_o[1:2], 1)
        for k in range(K):
            crow[b, k] = cmap[k * L : (k + 1) * L]
            brow_t[b, k] = jnp.transpose(bmap[k * L : (k + 1) * L].astype(F32)).astype(BF16)
        value_conv(0, b)
    for b in range(B):
        value_dot(1, b)
        for k in range(K):
            sc[b, k] = jnp.where(tri, dot(crow[b, k], brow_t[b, k]), 0.0).astype(BF16)
        value_state(0, b)
    for g in range(G):
        g_copy(g).start()

    for g in range(2, G):
        v_copy(g).wait()
        send_shares(g - 2)
        for b in range(B):
            value_conv(g - 1, b)
        for b in range(B):
            value_dot(g, b)
            value_state(g - 1, b)

    def arrived(lump):
        bulk(recvbuf, lump, ssem, rsem).wait_recv()

    def returned(lump):
        bulk(retrecv, lump, tsem, usem).wait_recv()

    g_copy(0).wait()
    arrived(0)
    send_shares(3)
    my_half = lax.rem(me // 8, 2)
    through = recvbuf[:, 0].reshape(PEERS * 16, 128)
    for g in range(G):
        fac[g] = dot(through, eh[my_half, g]).reshape(PEERS, 16, 128)
    chain_share(0)
    for b in range(B):
        value_conv(4, b)
    for b in range(B):
        gate_dot(0, b)
        value_state(4, b)

    g_copy(1).wait()
    arrived(1)
    send_shares(4)
    chain_share(1)
    for b in range(B):
        gate_dot(1, b)
        within(b, 0)
        within(b, 1)

    g_copy(2).wait()
    arrived(2)
    arrived(3)
    chain_share(2)
    chain_share(3)
    for b in range(B):
        gate_dot(2, b)
        within(2 + b, 0)
        within(2 + b, 1)

    g_copy(3).wait()
    arrived(4)
    returned(0)
    chain_share(4)
    for b in range(B):
        carry(0, b)
        gate_dot(3, b)
        within(4, b)

    g_copy(4).wait()
    returned(1)
    returned(2)
    for b in range(B):
        carry(1 + b, 0)
        gate_dot(4, b)
        carry(1 + b, 1)

    returned(3)
    returned(4)
    for b in range(B):
        carry(3, b)
        carry(4, b)

    ones = jnp.ones((8, 256), BF16)
    for b in range(B):
        hi, mid, _ = split3(sq[b])
        terms = jnp.concatenate([hi, mid], axis=1).astype(BF16)
        ssend[b] = lax.dot_general(ones, terms, (((1,), (1,)), ((), ())), preferred_element_type=F32)

    def square_copy(d):
        return pltpu.make_async_remote_copy(
            src_ref=ssend,
            dst_ref=srecv.at[hd],
            send_sem=qsem.at[0],
            recv_sem=qsem.at[1],
            device_id={"head": lax.rem(hd + d, HEADS_AXIS)},
            device_id_type=MESH,
        )

    for d in range(1, HEADS_AXIS):
        square_copy(d).start()
    srecv[hd] = ssend[...]
    pltpu.make_async_remote_copy(
        src_ref=srecv.at[pl.ds(0, HEADS_AXIS - 1)],
        dst_ref=srecv.at[pl.ds(0, HEADS_AXIS - 1)],
        send_sem=qsem.at[0],
        recv_sem=qsem.at[1],
        device_id={"head": hd},
        device_id_type=MESH,
    ).wait_recv()
    eighth = jnp.full((16, 128), 0.125, BF16)
    for b in range(B):
        total = srecv[0, b] + srecv[1, b] + srecv[2, b] + srecv[3, b]
        inverse = lax.rsqrt(total / INNER + EPS)
        hi, mid, _ = split3(inverse)
        terms = jnp.concatenate([hi, mid], axis=0).astype(BF16)
        inverse_out[b] = lax.dot_general(terms, eighth, (((0,), (0,)), ((), ())), preferred_element_type=F32)

    for lump in range(G):
        bulk(sendbuf, lump, ssem, rsem).wait_send()
        bulk(retbuf, lump, tsem, usem).wait_send()
    pltpu.make_async_remote_copy(
        src_ref=srecv.at[pl.ds(0, HEADS_AXIS - 1)],
        dst_ref=srecv.at[pl.ds(0, HEADS_AXIS - 1)],
        send_sem=qsem.at[0],
        recv_sem=qsem.at[1],
        device_id={"head": hd},
        device_id_type=MESH,
    ).wait_send()

    @pl.when(me < PEERS - 1)
    def _():
        halo_copy(me + 1).wait_send()


def scale(gated, inverse, gain, out, obuf, sem):
    copies = []
    for b in range(B):
        for k in range(K):
            rows = slice(k * L, (k + 1) * L)
            factor = inverse[b, rows]
            for g in range(G):
                for j in range(2):
                    first = g * GC + j * 128
                    obuf[b, rows, first : first + 128] = (
                        gated[g, b, rows, j * 128 : (j + 1) * 128]
                        * factor
                        * gain[2 * g + j : 2 * g + j + 1]
                    ).astype(BF16)
            copies.append(
                pltpu.make_async_copy(
                    obuf.at[b, pl.ds(k * L, L)], out.at[b, pl.ds(k * L, L)], sem.at[b, k]
                )
            )
            copies[-1].start()
    for c in copies:
        c.wait()


def local_program(
    tokens, gate_weight, value_weight, state_weight, step_weight, value_kernel, value_offset,
    state_kernel, state_offset, step_offset, decay_rate, skip_gain, norm_gain,
):
    anywhere = pl.BlockSpec(memory_space=pl.ANY)
    inside = pl.BlockSpec(memory_space=pltpu.VMEM)
    vm = pltpu.VMEM
    dma = pltpu.SemaphoreType.DMA
    gated, inverse = pl.pallas_call(
        body,
        out_shape=(vm((G, B, T, GC), F32), vm((B, T, 128), F32)),
        in_specs=[anywhere] * 12,
        out_specs=(inside, inside),
        scratch_shapes=[
            vm((TAPS, C), F32),
            vm((C // 128, 128), F32),
            vm((TAPS, 2 * N), F32),
            vm((2, N), F32),
            vm((1, H), F32),
            vm((1, H), F32),
            vm((1, H), F32),
            vm((B, R, D), BF16),
            vm((G, D, GC), BF16),
            vm((G, D, GC), BF16),
            vm((D, 2 * N), BF16),
            vm((H, D), BF16),
            vm((B, 2, R, 128), F32),
            vm((B, 2, R, 128), F32),
            vm((G, B, T, GC), BF16),
            vm((G, B, T, GC), BF16),
            vm((B, K, N, L), BF16),
            vm((B, K, L, N), BF16),
            vm((B, K, L, L), BF16),
            vm((B, K, L, 128), F32),
            vm((B, K, L, 128), F32),
            vm((B, K, L, 128), BF16),
            vm((B, K, 32, L), F32),
            vm((G, 128, 256), BF16),
            vm((2, G, 128, 128), BF16),
            vm((G, 8, GC), F32),
            vm((G, 8, GC), F32),
            vm((G, 8, GC), F32),
            vm((40, 128), F32),
            vm((G, B, K - 1, N, GC), F32),
            vm((PEERS, G + 1, 16, 128), BF16),
            vm((PEERS, G + 1, 16, 128), BF16),
            vm((PEERS, G + 1, 16, 128), BF16),
            vm((PEERS, G + 1, 16, 128), BF16),
            vm((G, PEERS, 16, 128), F32),
            vm((B, T, 128), F32),
            vm((B, 8, T), F32),
            vm((HEADS_AXIS, B, 8, T), F32),
            dma((B,)), dma((G,)), dma((G,)), dma((2,)), dma((7,)), dma((2,)),
            dma((G,)), dma((G,)), dma((G,)), dma((G,)), dma((2,)),
        ],
        compiler_params=pltpu.CompilerParams(
            collective_id=0, has_side_effects=True, vmem_limit_bytes=50 * 1024 * 1024
        ),
        name="mixer",
    )(
        tokens, gate_weight, value_weight, state_weight, step_weight.T, value_kernel,
        value_offset.reshape(C // 128, 128), state_kernel, state_offset.reshape(2, N),
        step_offset.reshape(1, H), decay_rate.reshape(1, H), skip_gain.reshape(1, H),
    )
    return pl.pallas_call(
        scale,
        out_shape=jax.ShapeDtypeStruct((B, T, C), BF16),
        in_specs=[inside] * 3,
        out_specs=anywhere,
        scratch_shapes=[vm((B, T, C), BF16), dma((B, K))],
        compiler_params=pltpu.CompilerParams(vmem_limit_bytes=8 * 1024 * 1024),
        name="scale",
    )(gated, inverse, norm_gain.reshape(C // 128, 128))


def solution(mesh):
    return jax.shard_map(
        local_program,
        mesh=mesh,
        in_specs=(
            P(None, "seq", None),
            P(None, "head"),
            P(None, "head"),
            P(),
            P(None, "head"),
            P(None, "head"),
            P("head"),
            P(),
            P(),
            P("head"),
            P("head"),
            P("head"),
            P("head"),
        ),
        out_specs=P(None, "seq", "head"),
        check_vma=False,
    )
```
